256 devices in a mesh: seq: 64 (over x, z, y_lo), head: 4 (over y_hi, core).
Axes of the slice: x: 4, y: 4 (y_hi: 2, y_lo: 2; y = y_hi * 2 + y_lo), z: 8, core: 2. Of those that a mesh axis runs over, the one named last changes fastest.
Arguments:
- queries: bfloat16 [2, 512, 8192], P(None, 'seq', 'head'), may hold values from -256 to 256
- keys: bfloat16 [2, 16384, 1024], P(None, 'seq', 'head'), may hold values from -12 to 12
- lengths: int32 [2], replicated, may hold values from 768 to 16384, as said below
- starts: int32 [2], replicated, may hold values from 0 to 2048, as said below
Outputs:
- key_scores: float32 [2, 8, 16384], P(None, 'head', 'seq')
- token_scores: float32 [2, 16384], P(None, 'seq')
The draws below stay inside these ranges and needn't reach their ends.
Inputs may be any that keep to these rules, and one draw needn't show every extreme that they name: `lengths`: every length is a multiple of 128 and at least 768; in every draw one request has length 16384. `starts`: each start is at most its request's length minus 512 minus 128; in every draw one start equals 2048.
All inputs are finite; a program needn't handle non-finite values.
Results may differ from the reference program's by a relative error of at most 0.0003.
Values may be sent and summed in bfloat16 or wider, within the bound.
A program may use at most 64 MiB of HBM per device.

```python
import jax
import jax.numpy as jnp
from jax import lax

H = 64
KVH = 8
D = 128
QLEN = 512
REQS = 2
CTX = 16384


def integer_draws(key):
    key_len, key_full, key_start = jax.random.split(jax.random.fold_in(key, 7), 3)
    lowest_block = (QLEN + 256 + 127) // 128
    highest_block = CTX // 128
    blocks = jax.random.randint(key_len, (REQS,), lowest_block, max(highest_block, lowest_block + 1))
    full_request = jax.random.randint(key_full, (), 0, REQS)
    is_full = jnp.arange(REQS) == full_request
    blocks = jnp.where(is_full, highest_block, blocks)
    lengths = (blocks * 128).astype(jnp.int32)
    upper = jnp.minimum(CTX // 8, lengths - QLEN - 128)
    starts = jax.random.randint(key_start, (REQS,), 0, upper + 1)
    starts = jnp.where(is_full, CTX // 8, starts).astype(jnp.int32)
    return (lengths, starts)


def key_entries(key):
    entries = jax.random.normal(jax.random.fold_in(key, 21), (REQS, CTX, KVH, D), jnp.float32)
    entries = jnp.clip(entries, -6.0, 6.0)
    return entries


def draw_lengths(key, part):
    return integer_draws(key)[0]


def draw_starts(key, part):
    return integer_draws(key)[1]


def draw_keys(key, part):
    return key_entries(key).reshape(REQS, CTX, KVH * D).astype(jnp.bfloat16)


def draw_queries(key, part):
    entries = jax.random.normal(jax.random.fold_in(key, 31), (REQS, QLEN, H, D), jnp.float32)
    entries = jnp.clip(entries, -6.0, 6.0)
    return entries.reshape(REQS, QLEN, H * D).astype(jnp.bfloat16)


def setup_inputs(seed: int = 0) -> dict:
    splits = jax.random.split(jax.random.key(seed), 5)
    queries = draw_queries(jax.random.fold_in(splits[4], 71), 0)
    keys = draw_keys(jax.random.fold_in(splits[4], 71), 0)
    lengths = draw_lengths(jax.random.fold_in(splits[4], 71), 0)
    starts = draw_starts(jax.random.fold_in(splits[4], 71), 0)
    return {"queries": queries, "keys": keys, "lengths": lengths, "starts": starts}


MASK_FILL = -1e30


def reference(queries, keys, lengths, starts):
    group_size = H // KVH
    score_scale = D ** -0.5
    query_all = queries.reshape(REQS, QLEN, KVH, group_size, D)
    key_all = keys.reshape(REQS, CTX, KVH, D)
    key_pos = jnp.arange(CTX, dtype=jnp.int32)

    def column_sums_of(item_index):
        request_id = item_index // KVH
        head_id = item_index % KVH
        query_block = lax.dynamic_index_in_dim(query_all, request_id, 0, keepdims=False)
        query_block = lax.dynamic_index_in_dim(query_block, head_id, 1, keepdims=False)
        key_block = lax.dynamic_index_in_dim(key_all, request_id, 0, keepdims=False)
        key_block = lax.dynamic_index_in_dim(key_block, head_id, 1, keepdims=False)
        scores = jnp.einsum("thd,kd->htk", query_block.astype(jnp.float32), key_block.astype(jnp.float32),
                            precision=lax.Precision.HIGHEST) * score_scale
        length = lengths[request_id]
        start = starts[request_id]
        query_pos = length - QLEN + jnp.arange(QLEN, dtype=jnp.int32)
        allowed = (key_pos[None, :] <= query_pos[:, None]) & (key_pos[None, :] >= start)
        masked = jnp.where(allowed[None], scores, MASK_FILL)
        row_max = jnp.max(masked, axis=2, keepdims=True)
        expos = jnp.where(allowed[None], jnp.exp(masked - row_max), 0.0)
        row_sum = jnp.sum(expos, axis=2, keepdims=True)
        probs = expos / row_sum
        return jnp.sum(probs, axis=(0, 1))

    columns = lax.map(column_sums_of, jnp.arange(REQS * KVH, dtype=jnp.int32))
    key_scores = columns.reshape(REQS, KVH, CTX)
    token_scores = jnp.sum(key_scores, axis=1)
    return key_scores, token_scores
```

```python
import functools
import math

import jax
import jax.numpy as jnp
from jax import lax
from jax.experimental import pallas as pl
from jax.experimental.pallas import tpu as pltpu
from jax.sharding import Mesh
from jax.sharding import PartitionSpec as P

H = 64
KVH = 8
D = 128
QLEN = 512
SEQ = ("seq_0", "seq_1", "seq_2")
AXES = SEQ + ("head",)
NX, NZ, NY, NH = 4, 8, 2, 4
TOK = 8
KEYS = 256
HALF = H // KVH // NY
ROWS = NX * NY * TOK * HALF
BLOCKS = NX * NY
FILL = -1e30
SCALE2 = D**-0.5 * math.log2(math.e)
MESH = pl.DeviceIdType.MESH
PLANE = tuple((dx, dy) for dx in (2, 1, 3, 0) for dy in (1, 0) if (dx, dy) != (0, 0))
OFFSETS = (0, 1, -1, 2, -2, 3, -3, 4)
ARRIVAL = {off: j for j, off in enumerate(OFFSETS)}
PIECES = 2
PX = NX // PIECES


def wrap(value, size):
    return lax.rem(value + size, size)


def kernel(
    len_ref, start_ref, q_hbm, k_hbm, key_out, tok_out,
    qloc, kloc, qbuf, kbuf, sbuf, thr, mrow, wrow, lse, part, got, tok,
    loc_sem, qs, qr, ks, kr, zs, zr, ss, sr, ps, pr, ts, tr,
):
    x, z, y, hd = (lax.axis_index(a) for a in AXES)
    f32 = jnp.float32

    def share_of(ref, px, py):
        b, g = px // 2, lax.rem(px, 2)
        lanes = pl.multiple_of(g * (NY * HALF * D) + py * (HALF * D), HALF * D)
        return ref.at[b, :, pl.ds(lanes, HALF * D)]

    def keys_of(ref, px):
        b, g = px // 2, lax.rem(px, 2)
        return ref.at[b, :, pl.ds(pl.multiple_of(g * D, D), D)]

    local = [
        pltpu.make_async_copy(q_hbm, qloc, loc_sem.at[0]),
        pltpu.make_async_copy(k_hbm, kloc, loc_sem.at[1]),
        pltpu.make_async_copy(share_of(q_hbm, x, y), qbuf.at[z, x, y], loc_sem.at[2]),
        pltpu.make_async_copy(keys_of(k_hbm, x), kbuf.at[x, y], loc_sem.at[3]),
    ]
    for copy in local:
        copy.start()

    barrier = pltpu.get_barrier_semaphore()
    partners = [(wrap(x + dx, NX), z, wrap(y + dy, NY), hd) for dx, dy in PLANE]
    partners += [(x, wrap(z + dz, NZ), y, hd) for dz in (2, -2, 1, -1)]
    partners += [(x, z, y, wrap(hd + dh, NH)) for dh in range(1, NH)]
    for partner in partners:
        pl.semaphore_signal(barrier, inc=1, device_id=partner, device_id_type=MESH)
    local[0].wait()
    local[1].wait()
    pl.semaphore_wait(barrier, len(partners))

    def remote(src, dst, send, recv, device):
        return pltpu.make_async_remote_copy(
            src_ref=src, dst_ref=dst, send_sem=send, recv_sem=recv,
            device_id=device, device_id_type=MESH,
        )

    started = []

    def start(copy):
        copy.start()
        started.append(copy)

    for n, (dx, dy) in enumerate(PLANE):
        px, py = wrap(x + dx, NX), wrap(y + dy, NY)
        start(remote(share_of(qloc, px, py), qbuf.at[z, x, y], qs.at[n], qr.at[x, y], (px, z, py, hd)))
    for n, (dx, dy) in enumerate(PLANE):
        px, py = wrap(x + dx, NX), wrap(y + dy, NY)
        start(remote(keys_of(kloc, px), kbuf.at[x, y], ks.at[n], kr.at[x, y], (px, z, py, hd)))

    b = x // 2
    start_pos = start_ref[b]
    for px in range(NX):
        for py in range(NY):
            pos = ((px * NZ + z) * NY + py) * KEYS + lax.broadcasted_iota(jnp.int32, (KEYS, D), 0)
            thr[px * NY + py] = jnp.where(pos >= start_pos, pos, jnp.int32(2**30))

    def z_copy(off, piece, dz, n):
        slot = wrap(z + off, NZ)
        rows = pl.ds(piece * PX, PX)
        there = off - dz
        j = ARRIVAL[there] if there in ARRIVAL else ARRIVAL[-there]
        return remote(
            qbuf.at[slot, rows], qbuf.at[slot, rows], zs.at[n], zr.at[j, piece],
            (x, wrap(z + dz, NZ), y, hd),
        )

    def z_wait(off, piece):
        slot = wrap(z + off, NZ)
        rows = pl.ds(piece * PX, PX)
        remote(
            qbuf.at[slot, rows], qbuf.at[slot, rows], zs.at[0], zr.at[ARRIVAL[off], piece],
            (x, wrap(z + 1, NZ), y, hd),
        ).wait_recv()

    for dx, dy in PLANE:
        px, py = wrap(x + dx, NX), wrap(y + dy, NY)
        remote(
            share_of(qloc, px, py), qbuf.at[z, px, py], qs.at[0], qr.at[px, py], (px, z, py, hd)
        ).wait_recv()
    local[2].wait()
    sends = 0
    for piece in range(PIECES):
        for dz in (1, -1):
            start(z_copy(0, piece, dz, sends))
            sends += 1
    for hop in (1, 2):
        for piece in range(PIECES):
            for side in (1, -1):
                z_wait(side * hop, piece)
                start(z_copy(side * hop, piece, -side, sends))
                sends += 1
                if hop == 2 and piece == (0 if side == -1 else PIECES - 1):
                    start(z_copy(side * hop, piece, -2 * side, sends))
                    sends += 1

    local[3].wait()
    for dx, dy in PLANE:
        px, py = wrap(x + dx, NX), wrap(y + dy, NY)
        remote(
            keys_of(kloc, px), kbuf.at[px, py], ks.at[0], kr.at[px, py], (px, z, py, hd)
        ).wait_recv()

    first_pos = len_ref[b] - QLEN

    def score(off):
        c = wrap(z + off, NZ)
        wide = qbuf[c].astype(f32).reshape(BLOCKS * TOK, HALF * D)
        q = jnp.concatenate([wide[:, h * D:(h + 1) * D] for h in range(HALF)], axis=0).astype(jnp.bfloat16)
        lane = lax.rem(lax.broadcasted_iota(jnp.int32, (1, ROWS), 1), BLOCKS * TOK)
        inner = NY * TOK
        query_pos = first_pos + (lane // inner) * (NZ * inner) + c * inner + lax.rem(lane, inner)

        def scores(n, top):
            s = lax.dot_general(
                kbuf[n // NY, lax.rem(n, NY)], q, (((1,), (1,)), ((), ())), preferred_element_type=f32
            )
            limit = thr[n]
            s = jnp.where(jnp.concatenate([limit, limit], axis=1) <= query_pos, s, FILL)
            sbuf[c, n] = s
            return jnp.maximum(top, jnp.max(s.reshape(KEYS // 8, 8, ROWS), axis=0))

        top = lax.fori_loop(0, BLOCKS, scores, jnp.full((8, ROWS), FILL, f32))
        top = jnp.max(top, axis=0, keepdims=True)

        def expos(n, total):
            e = jnp.exp2((sbuf[c, n] - top) * SCALE2)
            sbuf[c, n] = e
            return total + jnp.sum(e.reshape(KEYS // 8, 8, ROWS), axis=0)

        total = lax.fori_loop(0, BLOCKS, expos, jnp.zeros((8, ROWS), f32))
        total = jnp.sum(total, axis=0, keepdims=True)
        top = top * SCALE2
        mrow[pl.ds(c, 1), :] = top
        lse[z, pl.ds(c, 1), :] = top + jnp.log2(total)

    for off in OFFSETS:
        if abs(off) > 2:
            for piece in range(PIECES):
                z_wait(off, piece)
        score(off)

    def stats(dz, n):
        return remote(lse.at[z], lse.at[z], ss.at[n], sr.at[z], (x, wrap(z + dz, NZ), y, hd))

    for n, dz in enumerate((4, 3, -3, 2, -2, 1, -1)):
        start(stats(dz, n))
    for n, dz in enumerate((1, -1, 2, -2, 3, -3, 4)):
        other = wrap(z + dz, NZ)
        remote(lse.at[other], lse.at[other], ss.at[0], sr.at[other], (x, other, y, hd)).wait_recv()
    every = [lse[k] for k in range(NZ)]
    peak = functools.reduce(jnp.maximum, every)
    whole = peak + jnp.log2(sum(jnp.exp2(v - peak) for v in every))
    wrow[...] = jnp.exp2(mrow[...] - whole)

    ones = jnp.ones((16, D), jnp.bfloat16)
    order = PLANE + ((0, 0),)
    for n, (dx, dy) in enumerate(order):
        px, py = wrap(x + dx, NX), wrap(y + dy, NY)
        block = px * NY + py

        def weigh(c, acc):
            w = wrow[pl.ds(c, 1), :]
            e = sbuf[c, block] * w
            return acc + e[:, :D] + e[:, D:]

        acc = lax.fori_loop(0, NZ, weigh, jnp.zeros((KEYS, D), f32))
        hi = acc.astype(jnp.bfloat16)
        rest = acc - hi.astype(f32)
        mid = rest.astype(jnp.bfloat16)
        low = (rest - mid.astype(f32)).astype(jnp.bfloat16)
        sums = sum(
            lax.dot_general(ones, v, (((1,), (1,)), ((), ())), preferred_element_type=f32)
            for v in (low, mid, hi)
        )[0:1]
        if (dx, dy) == (0, 0):
            got[x, y] = sums
        else:
            part[n] = sums
            start(remote(part.at[n], got.at[x, y], ps.at[n], pr.at[x, y], (px, z, py, hd)))
    for n, (dx, dy) in enumerate(PLANE):
        px, py = wrap(x + dx, NX), wrap(y + dy, NY)
        remote(part.at[n], got.at[px, py], ps.at[n], pr.at[px, py], (px, z, py, hd)).wait_recv()

    heads = KVH // NH
    for request in range(2):
        sums = []
        for g in range(heads):
            pair = request * heads + g
            sums.append(got[pair, 0] + got[pair, 1])
            key_out[request, g:g + 1] = sums[-1]
        tok[hd, request] = sum(sums[1:], sums[0])
    for dh in range(1, NH):
        start(remote(tok.at[hd], tok.at[hd], ts.at[dh], tr.at[hd], (x, z, y, wrap(hd + dh, NH))))
    for dh in range(1, NH):
        other = wrap(hd + dh, NH)
        remote(tok.at[other], tok.at[other], ts.at[dh], tr.at[other], (x, z, y, other)).wait_recv()
    for request in range(2):
        tok_out[request:request + 1] = sum((tok[k, request] for k in range(1, NH)), tok[0, request])

    for copy in started:
        copy.wait_send()


def body(queries, keys, lengths, starts):
    f32, bf16 = jnp.float32, jnp.bfloat16
    dma = pltpu.SemaphoreType.DMA
    vmem = pltpu.VMEM
    return pl.pallas_call(
        kernel,
        out_shape=(
            jax.ShapeDtypeStruct((2, KVH // NH, KEYS), f32),
            jax.ShapeDtypeStruct((2, KEYS), f32),
        ),
        in_specs=[pl.BlockSpec(memory_space=pltpu.SMEM)] * 2
        + [pl.BlockSpec(memory_space=pltpu.HBM)] * 2,
        out_specs=(pl.BlockSpec(memory_space=vmem), pl.BlockSpec(memory_space=vmem)),
        scratch_shapes=[
            vmem(queries.shape, bf16),
            vmem(keys.shape, bf16),
            vmem((NZ, NX, NY, TOK, HALF * D), bf16),
            vmem((NX, NY, KEYS, D), bf16),
            vmem((NZ, BLOCKS, KEYS, ROWS), f32),
            vmem((BLOCKS, KEYS, D), jnp.int32),
            vmem((NZ, ROWS), f32),
            vmem((NZ, ROWS), f32),
            vmem((NZ, NZ, ROWS), f32),
            vmem((len(PLANE), 1, KEYS), f32),
            vmem((NX, NY, 1, KEYS), f32),
            vmem((NH, 2, 1, KEYS), f32),
            dma((4,)),
            dma((len(PLANE),)), dma((NX, NY)),
            dma((len(PLANE),)), dma((NX, NY)),
            dma((6 * PIECES + 2,)), dma((NZ, PIECES)),
            dma((NZ - 1,)), dma((NZ,)),
            dma((len(PLANE),)), dma((NX, NY)),
            dma((NH,)), dma((NH,)),
        ],
        compiler_params=pltpu.CompilerParams(
            collective_id=0, has_side_effects=True, vmem_limit_bytes=48 * 1024 * 1024
        ),
        name="key_scores",
    )(lengths, starts, queries, keys)


def solution(mesh):
    torus = Mesh(mesh.devices.reshape(NX, NZ, NY, NH), AXES)
    in_specs = (P(None, SEQ, "head"), P(None, SEQ, "head"), P(), P())
    out_specs = (P(None, "head", SEQ), P(None, SEQ))
    return jax.shard_map(body, mesh=torus, in_specs=in_specs, out_specs=out_specs, check_vma=False)
```

```python
import functools
import math

import jax
import jax.numpy as jnp
from jax import lax
from jax.experimental import pallas as pl
from jax.experimental.pallas import tpu as pltpu
from jax.sharding import Mesh
from jax.sharding import PartitionSpec as P

H = 64
KVH = 8
D = 128
QLEN = 512
SEQ = ("seq_0", "seq_1", "seq_2")
AXES = SEQ + ("head",)
NX, NZ, NY, NH = 4, 8, 2, 4
TOK = 8
KEYS = 256
HALF = H // KVH // NY
ROWS = NX * NY * TOK * HALF
BLOCKS = NX * NY
FILL = -1e30
SCALE2 = D**-0.5 * math.log2(math.e)
MESH = pl.DeviceIdType.MESH
PLANE = tuple((dx, dy) for dx in (2, 1, 3, 0) for dy in (1, 0) if (dx, dy) != (0, 0))
OFFSETS = (0, 1, -1, 2, -2, 3, -3, 4)
ARRIVAL = {off: j for j, off in enumerate(OFFSETS)}
PIECES = 2
PX = NX // PIECES
FORWARD_AT = 1


def wrap(value, size):
    return lax.rem(value + size, size)


def kernel(
    len_hbm, start_hbm, q_hbm, k_hbm, key_out, tok_out,
    len_ref, start_ref, qloc, kloc, qbuf, kbuf, sbuf, thr, msub, lsub, lse, accs, part, got,
    loc_sem, qs, qr, ks, kr, zs, zr, ss, sr, ps, pr,
):
    x, z, y, hd = (lax.axis_index(a) for a in AXES)
    f32, bf16 = jnp.float32, jnp.bfloat16

    def share_of(ref, px, py):
        b, g = px // 2, lax.rem(px, 2)
        lanes = pl.multiple_of(g * (NY * HALF * D) + py * (HALF * D), HALF * D)
        return ref.at[b, :, pl.ds(lanes, HALF * D)]

    def keys_of(ref, px):
        b, g = px // 2, lax.rem(px, 2)
        return ref.at[b, :, pl.ds(pl.multiple_of(g * D, D), D)]

    local = [
        pltpu.make_async_copy(q_hbm, qloc, loc_sem.at[0]),
        pltpu.make_async_copy(k_hbm, kloc, loc_sem.at[1]),
        pltpu.make_async_copy(share_of(q_hbm, x, y), qbuf.at[z, x, y], loc_sem.at[2]),
        pltpu.make_async_copy(keys_of(k_hbm, x), kbuf.at[x * NY + y], loc_sem.at[3]),
        pltpu.make_async_copy(len_hbm, len_ref, loc_sem.at[4]),
        pltpu.make_async_copy(start_hbm, start_ref, loc_sem.at[5]),
    ]
    for copy in local:
        copy.start()

    barrier = pltpu.get_barrier_semaphore()
    partners = [(x, wrap(z + dz, NZ), y, hd) for dz in (2, -2, 1, -1)]
    partners += [
        (wrap(x + dx, NX), z, wrap(y + dy, NY), wrap(hd + dh, NH))
        for dx, dy in PLANE + ((0, 0),) for dh in range(NH) if (dx, dy, dh) != (0, 0, 0)
    ]
    for partner in partners:
        pl.semaphore_signal(barrier, inc=1, device_id=partner, device_id_type=MESH)
    for copy in local:
        copy.wait()
    pl.semaphore_wait(barrier, len(partners))

    def remote(src, dst, send, recv, device):
        return pltpu.make_async_remote_copy(
            src_ref=src, dst_ref=dst, send_sem=send, recv_sem=recv,
            device_id=device, device_id_type=MESH,
        )

    started = []

    def start(copy):
        copy.start()
        started.append(copy)

    for n, (dx, dy) in enumerate(PLANE):
        px, py = wrap(x + dx, NX), wrap(y + dy, NY)
        start(remote(share_of(qloc, px, py), qbuf.at[z, x, y], qs.at[n], qr.at[x, y], (px, z, py, hd)))
    for n, (dx, dy) in enumerate(PLANE):
        px, py = wrap(x + dx, NX), wrap(y + dy, NY)
        start(remote(keys_of(kloc, px), kbuf.at[x * NY + y], ks.at[n], kr.at[x, y], (px, z, py, hd)))

    b = x // 2
    start_pos = start_ref[b]
    first_pos = len_ref[b] - QLEN
    for px in range(NX):
        for py in range(NY):
            pos = ((px * NZ + z) * NY + py) * KEYS + lax.broadcasted_iota(jnp.int32, (KEYS, D), 0)
            thr[px * NY + py] = jnp.where(pos >= start_pos, pos, jnp.int32(2**30))

    def z_copy(off, piece, dz, n):
        slot = wrap(z + off, NZ)
        rows = pl.ds(piece * PX, PX)
        there = off - dz
        j = ARRIVAL[there] if there in ARRIVAL else ARRIVAL[-there]
        return remote(
            qbuf.at[slot, rows], qbuf.at[slot, rows], zs.at[n], zr.at[j, piece],
            (x, wrap(z + dz, NZ), y, hd),
        )

    def z_wait(off, piece):
        slot = wrap(z + off, NZ)
        rows = pl.ds(piece * PX, PX)
        remote(
            qbuf.at[slot, rows], qbuf.at[slot, rows], zs.at[0], zr.at[ARRIVAL[off], piece],
            (x, wrap(z + 1, NZ), y, hd),
        ).wait_recv()

    sends = [0]

    def z_start(off, piece, dz):
        start(z_copy(off, piece, dz, sends[0]))
        sends[0] += 1

    def z_forward(hop):
        for piece in range(PIECES):
            for side in (1, -1):
                z_wait(side * hop, piece)
                z_start(side * hop, piece, -side)
                if hop == 2 and piece == (0 if side == -1 else PIECES - 1):
                    z_start(side * hop, piece, -2 * side)

    for dx, dy in PLANE[::-1]:
        px, py = wrap(x + dx, NX), wrap(y + dy, NY)
        remote(
            share_of(qloc, px, py), qbuf.at[z, px, py], qs.at[0], qr.at[px, py], (px, z, py, hd)
        ).wait_recv()
    for piece in range(PIECES):
        for dz in (1, -1):
            z_start(0, piece, dz)
    z_forward(1)

    def rows_of(c):
        wide = qbuf[c].astype(f32).reshape(BLOCKS * TOK, HALF * D)
        q = jnp.concatenate([wide[:, h * D:(h + 1) * D] for h in range(HALF)], axis=0).astype(bf16)
        lane = lax.rem(lax.broadcasted_iota(jnp.int32, (1, ROWS), 1), BLOCKS * TOK)
        inner = NY * TOK
        return q, first_pos + (lane // inner) * (NZ * inner) + c * inner + lax.rem(lane, inner)

    def score(c, q, query_pos, n):
        s = lax.dot_general(kbuf[n], q, (((1,), (1,)), ((), ())), preferred_element_type=f32)
        limit = thr[n]
        s = jnp.where(jnp.concatenate([limit, limit], axis=1) <= query_pos, s, FILL)
        top = jnp.max(s, axis=0, keepdims=True)
        e = jnp.exp2((s - top) * SCALE2)
        sbuf[c, n] = e
        msub[c, pl.ds(n, 1), :] = top
        lsub[c, pl.ds(n, 1), :] = jnp.sum(e, axis=0, keepdims=True)

    def merge(c):
        tops = msub[c] * SCALE2
        top = jnp.max(tops, axis=0, keepdims=True)
        total = jnp.sum(lsub[c] * jnp.exp2(tops - top), axis=0, keepdims=True)
        lse[z, pl.ds(c, 1), :] = top + jnp.log2(total)

    q, query_pos = rows_of(z)
    score(z, q, query_pos, x * NY + y)
    for dx, dy in PLANE[::-1]:
        px, py = wrap(x + dx, NX), wrap(y + dy, NY)
        remote(
            keys_of(kloc, px), kbuf.at[px * NY + py], ks.at[0], kr.at[px, py], (px, z, py, hd)
        ).wait_recv()
        score(z, q, query_pos, px * NY + py)
    merge(z)
    for j, off in enumerate(OFFSETS):
        if off == 0:
            continue
        if off == FORWARD_AT:
            z_forward(2)
        if abs(off) > 2:
            for piece in range(PIECES):
                z_wait(off, piece)
        c = wrap(z + off, NZ)
        q, query_pos = rows_of(c)
        for n in range(BLOCKS):
            score(c, q, query_pos, n)
        merge(c)

    for n, dz in enumerate((4, 3, -3, 2, -2, 1, -1)):
        start(remote(lse.at[z], lse.at[z], ss.at[n], sr.at[z], (x, wrap(z + dz, NZ), y, hd)))
    for dz in (1, -1, 2, -2, 3, -3, 4):
        other = wrap(z + dz, NZ)
        remote(lse.at[other], lse.at[other], ss.at[0], sr.at[other], (x, other, y, hd)).wait_recv()
    every = [lse[k] for k in range(NZ)]
    peak = functools.reduce(jnp.maximum, every)
    whole = peak + jnp.log2(sum(jnp.exp2(v - peak) for v in every))
    for c in range(NZ):
        msub[c] = jnp.exp2(msub[c] * SCALE2 - whole[c:c + 1])

    def weigh(n, carry):
        for half in range(2):
            rows = pl.ds(half * D, D)
            acc = jnp.zeros((D, D), f32)
            for c in range(NZ):
                w = msub[c, pl.ds(n, 1), :]
                acc = acc + sbuf[c, n, rows, :D] * w[:, :D]
                acc = acc + sbuf[c, n, rows, D:] * w[:, D:]
            accs[n, rows] = acc
        return carry

    lax.fori_loop(0, BLOCKS, weigh, 0)
    ones = jnp.ones((16, D), bf16)
    for n in range(BLOCKS):
        acc = accs[n]
        hi = acc.astype(bf16)
        rest = acc - hi.astype(f32)
        mid = rest.astype(bf16)
        low = (rest - mid.astype(f32)).astype(bf16)
        sums = sum(
            lax.dot_general(ones, v, (((1,), (1,)), ((), ())), preferred_element_type=f32)
            for v in (low, mid, hi)
        )
        part[n] = sums[0:1]
    got[hd, x, y] = part[x * NY + y]
    owners = [
        (dx, dy, dh) for dx, dy in PLANE + ((0, 0),) for dh in range(NH) if (dx, dy, dh) != (0, 0, 0)
    ]
    for n, (dx, dy, dh) in enumerate(owners):
        px, py, ph = wrap(x + dx, NX), wrap(y + dy, NY), wrap(hd + dh, NH)
        start(remote(
            part.at[px * NY + py], got.at[hd, x, y], ps.at[n], pr.at[hd, x, y], (px, z, py, ph)
        ))
    for n, (dx, dy, dh) in enumerate(owners[::-1]):
        px, py, ph = wrap(x + dx, NX), wrap(y + dy, NY), wrap(hd + dh, NH)
        remote(
            part.at[px * NY + py], got.at[ph, px, py], ps.at[n], pr.at[ph, px, py], (px, z, py, ph)
        ).wait_recv()

    heads = KVH // NH
    for request in range(2):
        total = None
        for k in range(NH):
            for g in range(heads):
                pair = request * heads + g
                sums = got[k, pair, 0] + got[k, pair, 1]
                total = sums if total is None else total + sums
        tok_out[request:request + 1] = total
        for g in range(heads):
            pair = request * heads + g
            key_out[request, g:g + 1] = got[hd, pair, 0] + got[hd, pair, 1]

    for copy in started:
        copy.wait_send()


def body(queries, keys, lengths, starts):
    f32, bf16 = jnp.float32, jnp.bfloat16
    dma = pltpu.SemaphoreType.DMA
    vmem = pltpu.VMEM
    return pl.pallas_call(
        kernel,
        out_shape=(
            jax.ShapeDtypeStruct((2, KVH // NH, KEYS), f32),
            jax.ShapeDtypeStruct((2, KEYS), f32),
        ),
        in_specs=[pl.BlockSpec(memory_space=pltpu.HBM)] * 4,
        out_specs=(pl.BlockSpec(memory_space=vmem), pl.BlockSpec(memory_space=vmem)),
        scratch_shapes=[
            pltpu.SMEM((2,), jnp.int32),
            pltpu.SMEM((2,), jnp.int32),
            vmem(queries.shape, bf16),
            vmem(keys.shape, bf16),
            vmem((NZ, NX, NY, TOK, HALF * D), bf16),
            vmem((BLOCKS, KEYS, D), bf16),
            vmem((NZ, BLOCKS, KEYS, ROWS), f32),
            vmem((BLOCKS, KEYS, D), jnp.int32),
            vmem((NZ, BLOCKS, ROWS), f32),
            vmem((NZ, BLOCKS, ROWS), f32),
            vmem((NZ, NZ, ROWS), f32),
            vmem((BLOCKS, KEYS, D), f32),
            vmem((BLOCKS, 1, KEYS), f32),
            vmem((NH, NX, NY, 1, KEYS), f32),
            dma((6,)),
            dma((len(PLANE),)), dma((NX, NY)),
            dma((len(PLANE),)), dma((NX, NY)),
            dma((6 * PIECES + 2,)), dma((NZ, PIECES)),
            dma((NZ - 1,)), dma((NZ,)),
            dma((NH * BLOCKS - 1,)), dma((NH, NX, NY)),
        ],
        compiler_params=pltpu.CompilerParams(
            collective_id=0, has_side_effects=True, vmem_limit_bytes=67043328
        ),
        name="key_scores",
    )(lengths, starts, queries, keys)


def solution(mesh):
    torus = Mesh(mesh.devices.reshape(NX, NZ, NY, NH), AXES)
    in_specs = (P(None, SEQ, "head"), P(None, SEQ, "head"), P(), P())
    out_specs = (P(None, "head", SEQ), P(None, SEQ))
    return jax.shard_map(body, mesh=torus, in_specs=in_specs, out_specs=out_specs, check_vma=False)
```

```python
import functools
import math

import jax
import jax.numpy as jnp
from jax import lax
from jax.experimental import pallas as pl
from jax.experimental.pallas import tpu as pltpu
from jax.sharding import Mesh
from jax.sharding import PartitionSpec as P

H = 64
KVH = 8
D = 128
QLEN = 512
SEQ = ("seq_0", "seq_1", "seq_2")
AXES = SEQ + ("head",)
NX, NZ, NY, NH = 4, 8, 2, 4
TOK = 8
KEYS = 256
HALF = H // KVH // NY
ROWS = NX * NY * TOK * HALF
BLOCKS = NX * NY
FILL = -1e30
SCALE2 = D**-0.5 * math.log2(math.e)
MESH = pl.DeviceIdType.MESH
PLANE = tuple((dx, dy) for dx in (2, 1, 3, 0) for dy in (1, 0) if (dx, dy) != (0, 0))
OFFSETS = (0, 1, -1, 2, -2, 3, -3, 4)
ARRIVAL = {off: j for j, off in enumerate(OFFSETS)}
STRIDES = (0, 1, 3, 2)
NEAR = (0, 1, -1)
FORWARD_AT = 5


def wrap(value, size):
    return lax.rem(value + size, size)


def kernel(
    len_hbm, start_hbm, q_hbm, k_hbm, key_out, tok_out,
    len_ref, start_ref, qloc, kloc, qbuf, kbuf, sbuf, thr, msub, lsub, lse, part, got,
    loc_sem, qs, qr, ks, kr, zs, zr, ss, sr, ps, pr,
):
    x, z, y, hd = (lax.axis_index(a) for a in AXES)
    f32, bf16 = jnp.float32, jnp.bfloat16

    def share_of(ref, px, py):
        b, g = px // 2, lax.rem(px, 2)
        lanes = pl.multiple_of(g * (NY * HALF * D) + py * (HALF * D), HALF * D)
        return ref.at[b, :, pl.ds(lanes, HALF * D)]

    def keys_of(ref, px):
        b, g = px // 2, lax.rem(px, 2)
        return ref.at[b, :, pl.ds(pl.multiple_of(g * D, D), D)]

    local = [
        pltpu.make_async_copy(q_hbm, qloc, loc_sem.at[0]),
        pltpu.make_async_copy(k_hbm, kloc, loc_sem.at[1]),
        pltpu.make_async_copy(share_of(q_hbm, x, y), qbuf.at[z, x, y], loc_sem.at[2]),
        pltpu.make_async_copy(keys_of(k_hbm, x), kbuf.at[x * NY + y], loc_sem.at[3]),
        pltpu.make_async_copy(len_hbm, len_ref, loc_sem.at[4]),
        pltpu.make_async_copy(start_hbm, start_ref, loc_sem.at[5]),
    ]
    for copy in local:
        copy.start()

    barrier = pltpu.get_barrier_semaphore()
    everywhere = PLANE + ((0, 0),)
    partners = [(x, wrap(z + dz, NZ), y, hd) for dz in (2, -2)]
    partners += [
        (wrap(x + dx, NX), wrap(z + dz, NZ), wrap(y + dy, NY), hd)
        for dz in (1, -1) for dx, dy in everywhere
    ]
    partners += [
        (wrap(x + dx, NX), z, wrap(y + dy, NY), wrap(hd + dh, NH))
        for dx, dy in everywhere for dh in range(NH) if (dx, dy, dh) != (0, 0, 0)
    ]
    for partner in partners:
        pl.semaphore_signal(barrier, inc=1, device_id=partner, device_id_type=MESH)
    for copy in local:
        copy.wait()
    pl.semaphore_wait(barrier, len(partners))

    def remote(src, dst, send, recv, device):
        return pltpu.make_async_remote_copy(
            src_ref=src, dst_ref=dst, send_sem=send, recv_sem=recv,
            device_id=device, device_id_type=MESH,
        )

    started = []

    def start(copy, apart=True):
        copy.start()
        if apart:
            started.append(copy)

    sends = [0]
    for dz in NEAR:
        for dx, dy in PLANE if dz == 0 else everywhere:
            px, py = wrap(x + dx, NX), wrap(y + dy, NY)
            start(remote(
                share_of(qloc, px, py), qbuf.at[z, x, y], qs.at[sends[0]], qr.at[ARRIVAL[-dz], x, y],
                (px, wrap(z + dz, NZ), py, hd),
            ))
            sends[0] += 1

    def q_wait(off, dx):
        for dy in (0, 1):
            if (off, dx, dy) != (0, 0, 0):
                px, py, pz = wrap(x + dx, NX), wrap(y + dy, NY), wrap(z + off, NZ)
                remote(
                    share_of(qloc, px, py), qbuf.at[pz, px, py], qs.at[0], qr.at[ARRIVAL[off], px, py],
                    (px, wrap(z + 1, NZ), py, hd),
                ).wait_recv()

    for n, (dx, dy) in enumerate(PLANE):
        px, py = wrap(x + dx, NX), wrap(y + dy, NY)
        start(remote(keys_of(kloc, px), kbuf.at[x * NY + y], ks.at[n], kr.at[x, y], (px, z, py, hd)))

    b = x // 2
    start_pos = start_ref[b]
    first_pos = len_ref[b] - QLEN
    for px in range(NX):
        for py in range(NY):
            pos = ((px * NZ + z) * NY + py) * KEYS + lax.broadcasted_iota(jnp.int32, (KEYS, D), 0)
            thr[px * NY + py] = jnp.where(pos >= start_pos, pos, jnp.int32(2**30))

    def z_copy(off, i, dz, n):
        slot, px = wrap(z + off, NZ), wrap(x + STRIDES[i], NX)
        there = off - dz
        j = ARRIVAL[there] if there in ARRIVAL else ARRIVAL[-there]
        return remote(
            qbuf.at[slot, px], qbuf.at[slot, px], zs.at[n], zr.at[j, i], (x, wrap(z + dz, NZ), y, hd)
        )

    def z_wait(off, i):
        slot, px = wrap(z + off, NZ), wrap(x + STRIDES[i], NX)
        remote(
            qbuf.at[slot, px], qbuf.at[slot, px], zs.at[0], zr.at[ARRIVAL[off], i],
            (x, wrap(z + 1, NZ), y, hd),
        ).wait_recv()

    sends = [0]

    def z_start(off, i, dz):
        start(z_copy(off, i, dz, sends[0]))
        sends[0] += 1

    def z_forward(i):
        for side in (1, -1):
            z_wait(side * 2, i)
            if (i % 2 == 0) == (side == 1):
                z_start(side * 2, i, -2 * side)
            z_start(side * 2, i, -side)

    for i, dx in enumerate(STRIDES):
        for side in (1, -1):
            q_wait(side, dx)
            z_start(side, i, -side)
    for dx in STRIDES:
        q_wait(0, dx)

    def rows_of(c):
        wide = qbuf[c].astype(f32).reshape(BLOCKS * TOK, HALF * D)
        q = jnp.concatenate([wide[:, h * D:(h + 1) * D] for h in range(HALF)], axis=0).astype(bf16)
        lane = lax.rem(lax.broadcasted_iota(jnp.int32, (1, ROWS), 1), BLOCKS * TOK)
        inner = NY * TOK
        return q, first_pos + (lane // inner) * (NZ * inner) + c * inner + lax.rem(lane, inner)

    def score(c, q, query_pos, n):
        s = lax.dot_general(kbuf[n], q, (((1,), (1,)), ((), ())), preferred_element_type=f32)
        limit = thr[n]
        s = jnp.where(jnp.concatenate([limit, limit], axis=1) <= query_pos, s, FILL)
        top = jnp.max(s, axis=0, keepdims=True)
        e = jnp.exp2((s - top) * SCALE2)
        sbuf[c, n] = e
        msub[c, pl.ds(n, 1), :] = top
        lsub[c, pl.ds(n, 1), :] = jnp.sum(e, axis=0, keepdims=True)

    def merge(c):
        tops = msub[c] * SCALE2
        top = jnp.max(tops, axis=0, keepdims=True)
        total = jnp.sum(lsub[c] * jnp.exp2(tops - top), axis=0, keepdims=True)
        lse[z, pl.ds(c, 1), :] = top + jnp.log2(total)

    near = [(wrap(z + off, NZ),) + rows_of(wrap(z + off, NZ)) for off in NEAR]
    for n, (dx, dy) in enumerate(((0, 0),) + PLANE):
        px, py = wrap(x + dx, NX), wrap(y + dy, NY)
        if n > 0:
            remote(
                keys_of(kloc, px), kbuf.at[px * NY + py], ks.at[0], kr.at[px, py], (px, z, py, hd)
            ).wait_recv()
        for c, q, query_pos in near:
            score(c, q, query_pos, px * NY + py)
        if n == FORWARD_AT:
            for i in range(NX):
                z_forward(i)
    for offs in ((2, -2), (3, -3), (4,)):
        for off in offs:
            if abs(off) > 2:
                for i in range(NX):
                    z_wait(off, i)
        far = [(wrap(z + off, NZ),) + rows_of(wrap(z + off, NZ)) for off in offs]
        for c, q, query_pos in far:
            for n in range(BLOCKS):
                score(c, q, query_pos, n)
        if offs == (2, -2):
            for off in NEAR:
                merge(wrap(z + off, NZ))
        for off in offs:
            merge(wrap(z + off, NZ))

    for dz in (4, 3, -3, 2, -2, 1, -1):
        start(remote(lse.at[z], lse.at[z], ss.at[0], sr.at[0], (x, wrap(z + dz, NZ), y, hd)), False)
    others = lse.at[pl.ds(0, NZ - 1)]
    stats = remote(others, others, ss.at[0], sr.at[0], (x, wrap(z + 1, NZ), y, hd))
    stats.wait_recv()
    every = [lse[k] for k in range(NZ)]
    peak = functools.reduce(jnp.maximum, every)
    whole = peak + jnp.log2(sum(jnp.exp2(v - peak) for v in every))
    for c in range(NZ):
        msub[c] = jnp.exp2(msub[c] * SCALE2 - whole[c:c + 1])

    ones = jnp.ones((16, 2 * D), bf16)

    def weigh(n):
        parts = []
        for half in range(2):
            rows = pl.ds(half * D, D)
            acc = jnp.zeros((D, D), f32)
            for c in range(NZ):
                w = msub[c, pl.ds(n, 1), :]
                acc = acc + sbuf[c, n, rows, :D] * w[:, :D]
                acc = acc + sbuf[c, n, rows, D:] * w[:, D:]
            high = acc.astype(bf16)
            low = (acc - high.astype(f32)).astype(bf16)
            parts.append(jnp.concatenate([high, low], axis=1))
        return lax.dot_general(
            ones, jnp.concatenate(parts, axis=0), (((1,), (1,)), ((), ())), preferred_element_type=f32
        )[0:1]

    def send_sums(dx, dy, sums):
        px, py = wrap(x + dx, NX), wrap(y + dy, NY)
        if (dx, dy) == (0, 0):
            got[hd, x, y] = sums
        part[px * NY + py] = sums
        for dh in (2, 3, 1, 0):
            if (dx, dy, dh) != (0, 0, 0):
                start(remote(
                    part.at[px * NY + py], got.at[hd, x, y], ps.at[0], pr.at[0],
                    (px, z, py, wrap(hd + dh, NH)),
                ), False)

    held = None
    for dx, dy in everywhere:
        sums = weigh(wrap(x + dx, NX) * NY + wrap(y + dy, NY))
        if held is not None:
            send_sums(*held)
        held = (dx, dy, sums)
    send_sums(*held)
    every_sum = got.reshape(NH * BLOCKS, 1, KEYS).at[pl.ds(0, NH * BLOCKS - 1)]
    returned = remote(every_sum, every_sum, ps.at[0], pr.at[0], (x, wrap(z + 1, NZ), y, hd))
    returned.wait_recv()

    heads = KVH // NH
    for request in range(2):
        total = None
        for k in range(NH):
            for g in range(heads):
                pair = request * heads + g
                sums = got[k, pair, 0] + got[k, pair, 1]
                total = sums if total is None else total + sums
        tok_out[request:request + 1] = total
        for g in range(heads):
            pair = request * heads + g
            key_out[request, g:g + 1] = got[hd, pair, 0] + got[hd, pair, 1]

    for copy in started + [stats, returned]:
        copy.wait_send()


def body(queries, keys, lengths, starts):
    f32, bf16 = jnp.float32, jnp.bfloat16
    dma = pltpu.SemaphoreType.DMA
    vmem = pltpu.VMEM
    return pl.pallas_call(
        kernel,
        out_shape=(
            jax.ShapeDtypeStruct((2, KVH // NH, KEYS), f32),
            jax.ShapeDtypeStruct((2, KEYS), f32),
        ),
        in_specs=[pl.BlockSpec(memory_space=pltpu.HBM)] * 4,
        out_specs=(pl.BlockSpec(memory_space=vmem), pl.BlockSpec(memory_space=vmem)),
        scratch_shapes=[
            pltpu.SMEM((2,), jnp.int32),
            pltpu.SMEM((2,), jnp.int32),
            vmem(queries.shape, bf16),
            vmem(keys.shape, bf16),
            vmem((NZ, NX, NY, TOK, HALF * D), bf16),
            vmem((BLOCKS, KEYS, D), bf16),
            vmem((NZ, BLOCKS, KEYS, ROWS), f32),
            vmem((BLOCKS, KEYS, D), jnp.int32),
            vmem((NZ, BLOCKS, ROWS), f32),
            vmem((NZ, BLOCKS, ROWS), f32),
            vmem((NZ, NZ, ROWS), f32),
            vmem((BLOCKS, 1, KEYS), f32),
            vmem((NH, NX, NY, 1, KEYS), f32),
            dma((6,)),
            dma((3 * BLOCKS - 1,)), dma((3, NX, NY)),
            dma((len(PLANE),)), dma((NX, NY)),
            dma((5 * NX,)), dma((NZ, NX)),
            dma((1,)), dma((1,)),
            dma((1,)), dma((1,)),
        ],
        compiler_params=pltpu.CompilerParams(
            collective_id=0, has_side_effects=True, vmem_limit_bytes=67043328
        ),
        name="key_scores",
    )(lengths, starts, queries, keys)


def solution(mesh):
    torus = Mesh(mesh.devices.reshape(NX, NZ, NY, NH), AXES)
    in_specs = (P(None, SEQ, "head"), P(None, SEQ, "head"), P(), P())
    out_specs = (P(None, "head", SEQ), P(None, SEQ))
    return jax.shard_map(body, mesh=torus, in_specs=in_specs, out_specs=out_specs, check_vma=False)
```

```python
import functools
import math

import jax
import jax.numpy as jnp
from jax import lax
from jax.experimental import pallas as pl
from jax.experimental.pallas import tpu as pltpu
from jax.sharding import Mesh
from jax.sharding import PartitionSpec as P

H = 64
KVH = 8
D = 128
QLEN = 512
SEQ = ("seq_0", "seq_1", "seq_2")
AXES = SEQ + ("head",)
NX, NZ, NY, NH = 4, 8, 2, 4
TOK = 8
KEYS = 256
HALF = H // KVH // NY
ROWS = NX * NY * TOK * HALF
BLOCKS = NX * NY
FILL = -1e30
SCALE2 = D**-0.5 * math.log2(math.e)
MESH = pl.DeviceIdType.MESH
PLANE = tuple((dx, dy) for dx in (2, 1, 3, 0) for dy in (1, 0) if (dx, dy) != (0, 0))
OFFSETS = (0, 1, -1, 2, -2, 3, -3, 4)
ARRIVAL = {off: j for j, off in enumerate(OFFSETS)}
STRIDES = (0, 1, 3, 2)
NEAR = (0, 1, -1)
FORWARD_AT = (2, 2, 2, 2)
KEY_ORDER = ((0, 1), (3, 0), (1, 0), (3, 1), (1, 1), (2, 0), (2, 1))
FIRST_KEYS = KEY_ORDER[:3]


def wrap(value, size):
    return lax.rem(value + size, size)


def kernel(
    len_hbm, start_hbm, q_hbm, k_hbm, key_out, tok_out,
    len_ref, start_ref, qloc, kloc, qbuf, kbuf, sbuf, thr, msub, lsub, lse, part, got,
    loc_sem, ready, qs, qr, ks, kr, zs, zr, ss, sr, ps, pr,
):
    x, z, y, hd = (lax.axis_index(a) for a in AXES)
    f32, bf16 = jnp.float32, jnp.bfloat16

    def share_of(ref, px, py):
        b, g = px // 2, lax.rem(px, 2)
        lanes = pl.multiple_of(g * (NY * HALF * D) + py * (HALF * D), HALF * D)
        return ref.at[b, :, pl.ds(lanes, HALF * D)]

    def keys_of(ref, px):
        b, g = px // 2, lax.rem(px, 2)
        return ref.at[b, :, pl.ds(pl.multiple_of(g * D, D), D)]

    local = [
        pltpu.make_async_copy(q_hbm, qloc, loc_sem.at[0]),
        pltpu.make_async_copy(k_hbm, kloc, loc_sem.at[1]),
        pltpu.make_async_copy(share_of(q_hbm, x, y), qbuf.at[z, x, y], loc_sem.at[2]),
        pltpu.make_async_copy(keys_of(k_hbm, x), kbuf.at[x * NY + y], loc_sem.at[3]),
        pltpu.make_async_copy(len_hbm, len_ref, loc_sem.at[4]),
        pltpu.make_async_copy(start_hbm, start_ref, loc_sem.at[5]),
    ]
    for copy in local:
        copy.start()

    barrier = pltpu.get_barrier_semaphore()
    everywhere = PLANE + ((0, 0),)
    beside = [(x, wrap(z + dz, NZ), y, hd) for dz in (1, -1)]
    heads_here = [(x, z, y, wrap(hd + dh, NH)) for dh in range(1, NH)]
    partners = beside + [(wrap(x + dx, NX), z, wrap(y + dy, NY), hd) for dx, dy in PLANE] + heads_here
    for partner in partners:
        pl.semaphore_signal(barrier, inc=1, device_id=partner, device_id_type=MESH)
    local[0].wait()
    pl.semaphore_wait(barrier, len(partners))
    for partner in beside:
        pl.semaphore_signal(ready.at[0], inc=1, device_id=partner, device_id_type=MESH)
    for partner in heads_here:
        pl.semaphore_signal(ready.at[1], inc=1, device_id=partner, device_id_type=MESH)

    def remote(src, dst, send, recv, device):
        return pltpu.make_async_remote_copy(
            src_ref=src, dst_ref=dst, send_sem=send, recv_sem=recv,
            device_id=device, device_id_type=MESH,
        )

    started = []

    def start(copy, apart=True):
        copy.start()
        if apart:
            started.append(copy)

    sends = [0]

    def q_start(dz, dx, dy):
        px, py = wrap(x + dx, NX), wrap(y + dy, NY)
        start(remote(
            share_of(qloc, px, py), qbuf.at[z, x, y], qs.at[sends[0]], qr.at[ARRIVAL[-dz], x, y],
            (px, wrap(z + dz, NZ), py, hd),
        ))
        sends[0] += 1

    def k_start(dx, dy):
        px, py = wrap(x + dx, NX), wrap(y + dy, NY)
        n = PLANE.index((dx, dy))
        start(remote(keys_of(kloc, px), kbuf.at[x * NY + y], ks.at[n], kr.at[x, y], (px, z, py, hd)))

    for dx, dy in PLANE:
        q_start(0, dx, dy)
    for dz in (1, -1):
        q_start(dz, 0, 0)
    for copy in local[1:]:
        copy.wait()
    for dx, dy in FIRST_KEYS:
        k_start(dx, dy)
    pl.semaphore_wait(ready.at[0], len(beside))
    for dx, dy in PLANE:
        for dz in (1, -1):
            q_start(dz, dx, dy)
    for dx, dy in KEY_ORDER:
        if (dx, dy) not in FIRST_KEYS:
            k_start(dx, dy)

    def q_wait(off, dx):
        for dy in (0, 1):
            if (off, dx, dy) != (0, 0, 0):
                px, py, pz = wrap(x + dx, NX), wrap(y + dy, NY), wrap(z + off, NZ)
                remote(
                    share_of(qloc, px, py), qbuf.at[pz, px, py], qs.at[0], qr.at[ARRIVAL[off], px, py],
                    (px, wrap(z + 1, NZ), py, hd),
                ).wait_recv()

    b = x // 2
    start_pos = start_ref[b]
    first_pos = len_ref[b] - QLEN
    for px in range(NX):
        for py in range(NY):
            pos = ((px * NZ + z) * NY + py) * KEYS + lax.broadcasted_iota(jnp.int32, (KEYS, D), 0)
            thr[px * NY + py] = jnp.where(pos >= start_pos, pos, jnp.int32(2**30))

    def z_copy(off, i, dz, n):
        slot, px = wrap(z + off, NZ), wrap(x + STRIDES[i], NX)
        there = off - dz
        j = ARRIVAL[there] if there in ARRIVAL else ARRIVAL[-there]
        return remote(
            qbuf.at[slot, px], qbuf.at[slot, px], zs.at[n], zr.at[j, i], (x, wrap(z + dz, NZ), y, hd)
        )

    def z_wait(off, i):
        slot, px = wrap(z + off, NZ), wrap(x + STRIDES[i], NX)
        remote(
            qbuf.at[slot, px], qbuf.at[slot, px], zs.at[0], zr.at[ARRIVAL[off], i],
            (x, wrap(z + 1, NZ), y, hd),
        ).wait_recv()

    sends = [0]

    def z_start(off, i, dz):
        start(z_copy(off, i, dz, sends[0]))
        sends[0] += 1

    def z_forward(i):
        for side in (1, -1):
            z_wait(side * 2, i)
            if (i % 2 == 0) == (side == 1):
                z_start(side * 2, i, -2 * side)
            z_start(side * 2, i, -side)

    for i, dx in enumerate(STRIDES):
        for side in (1, -1):
            q_wait(side, dx)
            z_start(side, i, -side)
    for dx in STRIDES:
        q_wait(0, dx)

    def rows_of(c):
        wide = qbuf[c].astype(f32).reshape(BLOCKS * TOK, HALF * D)
        q = jnp.concatenate([wide[:, h * D:(h + 1) * D] for h in range(HALF)], axis=0).astype(bf16)
        lane = lax.rem(lax.broadcasted_iota(jnp.int32, (1, ROWS), 1), BLOCKS * TOK)
        inner = NY * TOK
        return q, first_pos + (lane // inner) * (NZ * inner) + c * inner + lax.rem(lane, inner)

    def score(c, q, query_pos, n):
        s = lax.dot_general(kbuf[n], q, (((1,), (1,)), ((), ())), preferred_element_type=f32)
        limit = thr[n]
        s = jnp.where(jnp.concatenate([limit, limit], axis=1) <= query_pos, s, FILL)
        top = jnp.max(s, axis=0, keepdims=True)
        e = jnp.exp2((s - top) * SCALE2)
        sbuf[c, n] = e
        msub[c, pl.ds(n, 1), :] = top
        lsub[c, pl.ds(n, 1), :] = jnp.sum(e, axis=0, keepdims=True)

    def merge(c):
        tops = msub[c] * SCALE2
        top = jnp.max(tops, axis=0, keepdims=True)
        total = jnp.sum(lsub[c] * jnp.exp2(tops - top), axis=0, keepdims=True)
        lse[z, pl.ds(c, 1), :] = top + jnp.log2(total)

    near = [(wrap(z + off, NZ),) + rows_of(wrap(z + off, NZ)) for off in NEAR]
    for n, (dx, dy) in enumerate(((0, 0),) + KEY_ORDER):
        px, py = wrap(x + dx, NX), wrap(y + dy, NY)
        if n > 0:
            remote(
                keys_of(kloc, px), kbuf.at[px * NY + py], ks.at[0], kr.at[px, py], (px, z, py, hd)
            ).wait_recv()
        for c, q, query_pos in near:
            score(c, q, query_pos, px * NY + py)
        for i in range(NX):
            if n == FORWARD_AT[i]:
                z_forward(i)
    for offs in ((2, -2), (3, -3), (4,)):
        for off in offs:
            if abs(off) > 2:
                for i in range(NX):
                    z_wait(off, i)
        far = [(wrap(z + off, NZ),) + rows_of(wrap(z + off, NZ)) for off in offs]
        for c, q, query_pos in far:
            for n in range(BLOCKS):
                score(c, q, query_pos, n)
        if offs == (2, -2):
            for off in NEAR:
                merge(wrap(z + off, NZ))
        for off in offs:
            merge(wrap(z + off, NZ))

    for dz in (4, 3, -3, 2, -2, 1, -1):
        start(remote(lse.at[z], lse.at[z], ss.at[0], sr.at[0], (x, wrap(z + dz, NZ), y, hd)), False)
    others = lse.at[pl.ds(0, NZ - 1)]
    stats = remote(others, others, ss.at[0], sr.at[0], (x, wrap(z + 1, NZ), y, hd))
    for copy in started:
        copy.wait_send()
    started.clear()
    pl.semaphore_wait(ready.at[1], len(heads_here))
    stats.wait_recv()
    every = [lse[k] for k in range(NZ)]
    peak = functools.reduce(jnp.maximum, every)
    whole = peak + jnp.log2(sum(jnp.exp2(v - peak) for v in every))
    for c in range(NZ):
        msub[c] = jnp.exp2(msub[c] * SCALE2 - whole[c:c + 1])

    ones = jnp.ones((16, 2 * D), bf16)

    def weigh(n):
        parts = []
        for half in range(2):
            rows = pl.ds(half * D, D)
            acc = jnp.zeros((D, D), f32)
            for c in range(NZ):
                w = msub[c, pl.ds(n, 1), :]
                acc = acc + sbuf[c, n, rows, :D] * w[:, :D]
                acc = acc + sbuf[c, n, rows, D:] * w[:, D:]
            high = acc.astype(bf16)
            low = (acc - high.astype(f32)).astype(bf16)
            parts.append(jnp.concatenate([high, low], axis=1))
        return lax.dot_general(
            ones, jnp.concatenate(parts, axis=0), (((1,), (1,)), ((), ())), preferred_element_type=f32
        )[0:1]

    def send_sums(dx, dy, sums):
        px, py = wrap(x + dx, NX), wrap(y + dy, NY)
        if (dx, dy) == (0, 0):
            got[hd, x, y] = sums
        part[px * NY + py] = sums
        for dh in (2, 3, 1, 0):
            if (dx, dy, dh) != (0, 0, 0):
                start(remote(
                    part.at[px * NY + py], got.at[hd, x, y], ps.at[0], pr.at[0],
                    (px, z, py, wrap(hd + dh, NH)),
                ), False)

    held = None
    for dx, dy in everywhere:
        sums = weigh(wrap(x + dx, NX) * NY + wrap(y + dy, NY))
        if held is not None:
            send_sums(*held)
        held = (dx, dy, sums)
    send_sums(*held)
    every_sum = got.reshape(NH * BLOCKS, 1, KEYS).at[pl.ds(0, NH * BLOCKS - 1)]
    returned = remote(every_sum, every_sum, ps.at[0], pr.at[0], (x, wrap(z + 1, NZ), y, hd))
    returned.wait_recv()

    heads = KVH // NH
    for request in range(2):
        total = None
        for k in range(NH):
            for g in range(heads):
                pair = request * heads + g
                sums = got[k, pair, 0] + got[k, pair, 1]
                total = sums if total is None else total + sums
        tok_out[request:request + 1] = total
        for g in range(heads):
            pair = request * heads + g
            key_out[request, g:g + 1] = got[hd, pair, 0] + got[hd, pair, 1]

    for copy in started + [stats, returned]:
        copy.wait_send()


def body(queries, keys, lengths, starts):
    f32, bf16 = jnp.float32, jnp.bfloat16
    dma = pltpu.SemaphoreType.DMA
    vmem = pltpu.VMEM
    return pl.pallas_call(
        kernel,
        out_shape=(
            jax.ShapeDtypeStruct((2, KVH // NH, KEYS), f32),
            jax.ShapeDtypeStruct((2, KEYS), f32),
        ),
        in_specs=[pl.BlockSpec(memory_space=pltpu.HBM)] * 4,
        out_specs=(pl.BlockSpec(memory_space=vmem), pl.BlockSpec(memory_space=vmem)),
        scratch_shapes=[
            pltpu.SMEM((2,), jnp.int32),
            pltpu.SMEM((2,), jnp.int32),
            vmem(queries.shape, bf16),
            vmem(keys.shape, bf16),
            vmem((NZ, NX, NY, TOK, HALF * D), bf16),
            vmem((BLOCKS, KEYS, D), bf16),
            vmem((NZ, BLOCKS, KEYS, ROWS), f32),
            vmem((BLOCKS, KEYS, D), jnp.int32),
            vmem((NZ, BLOCKS, ROWS), f32),
            vmem((NZ, BLOCKS, ROWS), f32),
            vmem((NZ, NZ, ROWS), f32),
            vmem((BLOCKS, 1, KEYS), f32),
            vmem((NH, NX, NY, 1, KEYS), f32),
            dma((6,)),
            pltpu.SemaphoreType.REGULAR((2,)),
            dma((3 * BLOCKS - 1,)), dma((3, NX, NY)),
            dma((len(PLANE),)), dma((NX, NY)),
            dma((5 * NX,)), dma((NZ, NX)),
            dma((1,)), dma((1,)),
            dma((1,)), dma((1,)),
        ],
        compiler_params=pltpu.CompilerParams(
            collective_id=0, has_side_effects=True, vmem_limit_bytes=67043328
        ),
        name="key_scores",
    )(lengths, starts, queries, keys)


def solution(mesh):
    torus = Mesh(mesh.devices.reshape(NX, NZ, NY, NH), AXES)
    in_specs = (P(None, SEQ, "head"), P(None, SEQ, "head"), P(), P())
    out_specs = (P(None, "head", SEQ), P(None, SEQ))
    return jax.shard_map(body, mesh=torus, in_specs=in_specs, out_specs=out_specs, check_vma=False)
```

```python
import functools
import math

import jax
import jax.numpy as jnp
from jax import lax
from jax.experimental import pallas as pl
from jax.experimental.pallas import tpu as pltpu
from jax.sharding import Mesh
from jax.sharding import PartitionSpec as P

H = 64
KVH = 8
D = 128
QLEN = 512
SEQ = ("seq_0", "seq_1", "seq_2")
AXES = SEQ + ("head",)
NX, NZ, NY, NH = 4, 8, 2, 4
TOK = 8
KEYS = 256
HALF = H // KVH // NY
ROWS = NX * NY * TOK * HALF
BLOCKS = NX * NY
TOKENS = BLOCKS * TOK
SHARE = D // TOKENS
FILL = -1e30
SCALE2 = D**-0.5 * math.log2(math.e)
MESH = pl.DeviceIdType.MESH
PLANE = tuple((dx, dy) for dx in (2, 1, 3, 0) for dy in (1, 0) if (dx, dy) != (0, 0))
OFFSETS = (0, 1, -1, 2, -2, 3, -3, 4)
ARRIVAL = {off: j for j, off in enumerate(OFFSETS)}
STRIDES = (0, 1, 3, 2)
NEAR = (0, 1, -1)
GROUPS = ((2,), (-2,), (3,), (-3,), (4,))
FORWARD_AT = (4, 4, 4, 4)
KEY_ORDER = ((0, 1), (3, 0), (1, 0), (3, 1), (1, 1), (2, 0), (2, 1))
FIRST_KEYS = KEY_ORDER[:3]


def wrap(value, size):
    return lax.rem(value + size, size)


def kernel(
    len_hbm, start_hbm, q_hbm, k_hbm, key_out, tok_out,
    len_ref, start_ref, qloc, kloc, qbuf, kbuf, sbuf, barred, hot, msub, lsub, lse, part, got,
    loc_sem, ready, qs, qr, ks, kr, zs, zr, ss, sr, ps, pr,
):
    x, z, y, hd = (lax.axis_index(a) for a in AXES)
    f32, bf16 = jnp.float32, jnp.bfloat16

    def share_of(ref, px, py):
        b, g = px // 2, lax.rem(px, 2)
        lanes = pl.multiple_of(g * (NY * HALF * D) + py * (HALF * D), HALF * D)
        return ref.at[b, :, pl.ds(lanes, HALF * D)]

    def keys_of(ref, px):
        b, g = px // 2, lax.rem(px, 2)
        return ref.at[b, :, pl.ds(pl.multiple_of(g * D, D), D)]

    local = [
        pltpu.make_async_copy(q_hbm, qloc, loc_sem.at[0]),
        pltpu.make_async_copy(k_hbm, kloc, loc_sem.at[1]),
        pltpu.make_async_copy(share_of(q_hbm, x, y), qbuf.at[z, x, y], loc_sem.at[2]),
        pltpu.make_async_copy(keys_of(k_hbm, x), kbuf.at[x * NY + y], loc_sem.at[3]),
        pltpu.make_async_copy(len_hbm, len_ref, loc_sem.at[4]),
        pltpu.make_async_copy(start_hbm, start_ref, loc_sem.at[5]),
    ]
    for copy in local:
        copy.start()

    barrier = pltpu.get_barrier_semaphore()
    everywhere = PLANE + ((0, 0),)
    beside = [(x, wrap(z + dz, NZ), y, hd) for dz in (1, -1)]
    heads_here = [(x, z, y, wrap(hd + dh, NH)) for dh in range(1, NH)]
    partners = beside + [(wrap(x + dx, NX), z, wrap(y + dy, NY), hd) for dx, dy in PLANE] + heads_here
    for partner in partners:
        pl.semaphore_signal(barrier, inc=1, device_id=partner, device_id_type=MESH)
    local[0].wait()
    pl.semaphore_wait(barrier, len(partners))
    for partner in beside:
        pl.semaphore_signal(ready.at[0], inc=1, device_id=partner, device_id_type=MESH)
    for partner in heads_here:
        pl.semaphore_signal(ready.at[1], inc=1, device_id=partner, device_id_type=MESH)

    def remote(src, dst, send, recv, device):
        return pltpu.make_async_remote_copy(
            src_ref=src, dst_ref=dst, send_sem=send, recv_sem=recv,
            device_id=device, device_id_type=MESH,
        )

    started = []

    def start(copy, apart=True):
        copy.start()
        if apart:
            started.append(copy)

    sends = [0]

    def q_start(dz, dx, dy):
        px, py = wrap(x + dx, NX), wrap(y + dy, NY)
        start(remote(
            share_of(qloc, px, py), qbuf.at[z, x, y], qs.at[sends[0]], qr.at[ARRIVAL[-dz], x, y],
            (px, wrap(z + dz, NZ), py, hd),
        ))
        sends[0] += 1

    def k_start(dx, dy):
        px, py = wrap(x + dx, NX), wrap(y + dy, NY)
        n = PLANE.index((dx, dy))
        start(remote(keys_of(kloc, px), kbuf.at[x * NY + y], ks.at[n], kr.at[x, y], (px, z, py, hd)))

    for dx, dy in PLANE:
        q_start(0, dx, dy)
    for dz in (1, -1):
        q_start(dz, 0, 0)
    for copy in local[1:]:
        copy.wait()
    for dx, dy in FIRST_KEYS:
        k_start(dx, dy)
    pl.semaphore_wait(ready.at[0], len(beside))
    for dx, dy in PLANE:
        for dz in (1, -1):
            q_start(dz, dx, dy)
    for dx, dy in KEY_ORDER:
        if (dx, dy) not in FIRST_KEYS:
            k_start(dx, dy)

    def q_wait(off, dx):
        for dy in (0, 1):
            if (off, dx, dy) != (0, 0, 0):
                px, py, pz = wrap(x + dx, NX), wrap(y + dy, NY), wrap(z + off, NZ)
                remote(
                    share_of(qloc, px, py), qbuf.at[pz, px, py], qs.at[0], qr.at[ARRIVAL[off], px, py],
                    (px, wrap(z + 1, NZ), py, hd),
                ).wait_recv()

    b = x // 2
    start_pos = start_ref[b]
    first_pos = len_ref[b] - QLEN
    lane = lax.broadcasted_iota(jnp.int32, (1, D), 1)
    token = lax.rem(lane, TOKENS)
    inner = NY * TOK
    lane_pos = first_pos + (token // inner) * (NZ * inner) + lax.rem(token, inner) + (lane // TOKENS) * inner

    def mask(n, carry):
        pos = (((n // NY) * NZ + z) * NY + lax.rem(n, NY)) * KEYS
        pos = pos + lax.broadcasted_iota(jnp.int32, (KEYS, D), 0)
        limit = jnp.where(pos >= start_pos, pos, jnp.int32(2**30))
        for m in range(NZ // SHARE):
            barred[m, n] = jnp.where(limit <= lane_pos + m * SHARE * inner, 0.0, FILL).astype(bf16)
        return carry

    lax.fori_loop(0, BLOCKS, mask, 0)
    row = lax.rem(lax.broadcasted_iota(jnp.int32, (ROWS, D), 0), TOKENS)
    for m in range(SHARE):
        column = lax.broadcasted_iota(jnp.int32, (ROWS, D), 1) - m * TOKENS
        hot[m] = jnp.where(row == column, 1.0, 0.0).astype(bf16)

    def z_copy(off, i, dz, n):
        slot, px = wrap(z + off, NZ), wrap(x + STRIDES[i], NX)
        there = off - dz
        j = ARRIVAL[there] if there in ARRIVAL else ARRIVAL[-there]
        return remote(
            qbuf.at[slot, px], qbuf.at[slot, px], zs.at[n], zr.at[j, i], (x, wrap(z + dz, NZ), y, hd)
        )

    def z_wait(off, i):
        slot, px = wrap(z + off, NZ), wrap(x + STRIDES[i], NX)
        remote(
            qbuf.at[slot, px], qbuf.at[slot, px], zs.at[0], zr.at[ARRIVAL[off], i],
            (x, wrap(z + 1, NZ), y, hd),
        ).wait_recv()

    sends = [0]

    def z_start(off, i, dz):
        start(z_copy(off, i, dz, sends[0]))
        sends[0] += 1

    def z_forward(i):
        for side in (1, -1):
            z_wait(side * 2, i)
            z_start(side * 2, i, -side)
        if i == NX - 1:
            for k in range(NX):
                side = 1 if k % 2 == 0 else -1
                z_start(side * 2, k, -2 * side)

    for i, dx in enumerate(STRIDES):
        for side in (1, -1):
            q_wait(side, dx)
            z_start(side, i, -side)
    for dx in STRIDES:
        q_wait(0, dx)

    def rows_of(c):
        wide = qbuf[c].astype(f32).reshape(BLOCKS * TOK, HALF * D)
        q = jnp.concatenate([wide[:, h * D:(h + 1) * D] for h in range(HALF)], axis=0).astype(bf16)
        return jnp.concatenate([q, hot[lax.rem(c, SHARE)]], axis=1)

    def score(c, q, n):
        k = jnp.concatenate([kbuf[n], barred[c // SHARE, n]], axis=1)
        s = lax.dot_general(k, q, (((1,), (1,)), ((), ())), preferred_element_type=f32)
        top = jnp.max(s, axis=0, keepdims=True)
        e = jnp.exp2((s - top) * SCALE2)
        sbuf[c, n] = e
        msub[c, pl.ds(n, 1), :] = top
        lsub[c, pl.ds(n, 1), :] = jnp.sum(e, axis=0, keepdims=True)

    def merge(c):
        tops = msub[c] * SCALE2
        top = jnp.max(tops, axis=0, keepdims=True)
        total = jnp.sum(lsub[c] * jnp.exp2(tops - top), axis=0, keepdims=True)
        lse[z, pl.ds(c, 1), :] = top + jnp.log2(total)

    near = [(wrap(z + off, NZ), rows_of(wrap(z + off, NZ))) for off in NEAR]
    for n, (dx, dy) in enumerate(((0, 0),) + KEY_ORDER):
        px, py = wrap(x + dx, NX), wrap(y + dy, NY)
        if n > 0:
            remote(
                keys_of(kloc, px), kbuf.at[px * NY + py], ks.at[0], kr.at[px, py], (px, z, py, hd)
            ).wait_recv()
        for c, q in near:
            score(c, q, px * NY + py)
        for i in range(NX):
            if n == FORWARD_AT[i]:
                z_forward(i)
    for offs in GROUPS:
        for off in offs:
            if abs(off) > 2:
                for i in range(NX):
                    z_wait(off, i)
        far = [(wrap(z + off, NZ), rows_of(wrap(z + off, NZ))) for off in offs]
        for c, q in far:
            for n in range(BLOCKS):
                score(c, q, n)
        if 2 in offs:
            for off in NEAR:
                merge(wrap(z + off, NZ))
        for off in offs:
            merge(wrap(z + off, NZ))

    for dz in (4, 3, -3, 2, -2, 1, -1):
        start(remote(lse.at[z], lse.at[z], ss.at[0], sr.at[0], (x, wrap(z + dz, NZ), y, hd)), False)
    others = lse.at[pl.ds(0, NZ - 1)]
    stats = remote(others, others, ss.at[0], sr.at[0], (x, wrap(z + 1, NZ), y, hd))
    for copy in started:
        copy.wait_send()
    started.clear()
    pl.semaphore_wait(ready.at[1], len(heads_here))
    stats.wait_recv()
    every = [lse[k] for k in range(NZ)]
    peak = functools.reduce(jnp.maximum, every)
    whole = peak + jnp.log2(sum(jnp.exp2(v - peak) for v in every))
    for c in range(NZ):
        msub[c] = jnp.exp2(msub[c] * SCALE2 - whole[c:c + 1])

    ones = jnp.ones((16, 2 * D), bf16)

    def weigh(n):
        parts = []
        for half in range(2):
            rows = pl.ds(half * D, D)
            acc = jnp.zeros((D, D), f32)
            for c in range(NZ):
                w = msub[c, pl.ds(n, 1), :]
                acc = acc + sbuf[c, n, rows, :D] * w[:, :D]
                acc = acc + sbuf[c, n, rows, D:] * w[:, D:]
            high = acc.astype(bf16)
            low = (acc - high.astype(f32)).astype(bf16)
            parts.append(jnp.concatenate([high, low], axis=1))
        return lax.dot_general(
            ones, jnp.concatenate(parts, axis=0), (((1,), (1,)), ((), ())), preferred_element_type=f32
        )[0:1]

    def send_sums(dx, dy, sums):
        px, py = wrap(x + dx, NX), wrap(y + dy, NY)
        if (dx, dy) == (0, 0):
            got[hd, x, y] = sums
        part[px * NY + py] = sums
        for dh in (2, 3, 1, 0):
            if (dx, dy, dh) != (0, 0, 0):
                start(remote(
                    part.at[px * NY + py], got.at[hd, x, y], ps.at[0], pr.at[0],
                    (px, z, py, wrap(hd + dh, NH)),
                ), False)

    held = None
    for dx, dy in everywhere:
        sums = weigh(wrap(x + dx, NX) * NY + wrap(y + dy, NY))
        if held is not None:
            send_sums(*held)
        held = (dx, dy, sums)
    send_sums(*held)
    every_sum = got.reshape(NH * BLOCKS, 1, KEYS).at[pl.ds(0, NH * BLOCKS - 1)]
    returned = remote(every_sum, every_sum, ps.at[0], pr.at[0], (x, wrap(z + 1, NZ), y, hd))
    returned.wait_recv()

    heads = KVH // NH
    for request in range(2):
        total = None
        for k in range(NH):
            for g in range(heads):
                pair = request * heads + g
                sums = got[k, pair, 0] + got[k, pair, 1]
                total = sums if total is None else total + sums
        tok_out[request:request + 1] = total
        for g in range(heads):
            pair = request * heads + g
            key_out[request, g:g + 1] = got[hd, pair, 0] + got[hd, pair, 1]

    for copy in started + [stats, returned]:
        copy.wait_send()


def body(queries, keys, lengths, starts):
    f32, bf16 = jnp.float32, jnp.bfloat16
    dma = pltpu.SemaphoreType.DMA
    vmem = pltpu.VMEM
    return pl.pallas_call(
        kernel,
        out_shape=(
            jax.ShapeDtypeStruct((2, KVH // NH, KEYS), f32),
            jax.ShapeDtypeStruct((2, KEYS), f32),
        ),
        in_specs=[pl.BlockSpec(memory_space=pltpu.HBM)] * 4,
        out_specs=(pl.BlockSpec(memory_space=vmem), pl.BlockSpec(memory_space=vmem)),
        scratch_shapes=[
            pltpu.SMEM((2,), jnp.int32),
            pltpu.SMEM((2,), jnp.int32),
            vmem(queries.shape, bf16),
            vmem(keys.shape, bf16),
            vmem((NZ, NX, NY, TOK, HALF * D), bf16),
            vmem((BLOCKS, KEYS, D), bf16),
            vmem((NZ, BLOCKS, KEYS, ROWS), f32),
            vmem((NZ // SHARE, BLOCKS, KEYS, D), bf16),
            vmem((SHARE, ROWS, D), bf16),
            vmem((NZ, BLOCKS, ROWS), f32),
            vmem((NZ, BLOCKS, ROWS), f32),
            vmem((NZ, NZ, ROWS), f32),
            vmem((BLOCKS, 1, KEYS), f32),
            vmem((NH, NX, NY, 1, KEYS), f32),
            dma((6,)),
            pltpu.SemaphoreType.REGULAR((2,)),
            dma((3 * BLOCKS - 1,)), dma((3, NX, NY)),
            dma((len(PLANE),)), dma((NX, NY)),
            dma((5 * NX,)), dma((NZ, NX)),
            dma((1,)), dma((1,)),
            dma((1,)), dma((1,)),
        ],
        compiler_params=pltpu.CompilerParams(
            collective_id=0, has_side_effects=True, vmem_limit_bytes=67043328
        ),
        name="key_scores",
    )(lengths, starts, queries, keys)


def solution(mesh):
    torus = Mesh(mesh.devices.reshape(NX, NZ, NY, NH), AXES)
    in_specs = (P(None, SEQ, "head"), P(None, SEQ, "head"), P(), P())
    out_specs = (P(None, "head", SEQ), P(None, SEQ))
    return jax.shard_map(body, mesh=torus, in_specs=in_specs, out_specs=out_specs, check_vma=False)
```

```python
import functools
import math

import jax
import jax.numpy as jnp
from jax import lax
from jax.experimental import pallas as pl
from jax.experimental.pallas import tpu as pltpu
from jax.sharding import Mesh
from jax.sharding import PartitionSpec as P

H = 64
KVH = 8
D = 128
QLEN = 512
SEQ = ("seq_0", "seq_1", "seq_2")
AXES = SEQ + ("head",)
NX, NZ, NY, NH = 4, 8, 2, 4
TOK = 8
KEYS = 256
HALF = H // KVH // NY
ROWS = NX * NY * TOK * HALF
BLOCKS = NX * NY
TOKENS = BLOCKS * TOK
SHARE = D // TOKENS
FILL = -1e30
SCALE2 = D**-0.5 * math.log2(math.e)
MESH = pl.DeviceIdType.MESH
PLANE = tuple((dx, dy) for dx in (2, 1, 3, 0) for dy in (1, 0) if (dx, dy) != (0, 0))
OFFSETS = (0, 1, -1, 2, -2, 3, -3, 4)
ARRIVAL = {off: j for j, off in enumerate(OFFSETS)}
STRIDES = (0, 1, 3, 2)
NEAR = (0, 1, -1)
GROUPS = ((2,), (-2,), (3,), (-3,), (4,))
FORWARD_AT = (4, 4, 4, 4)
KEY_ORDER = ((0, 1), (3, 0), (1, 0), (3, 1), (1, 1), (2, 0), (2, 1))
FIRST_KEYS = KEY_ORDER[:3]


def wrap(value, size):
    return lax.rem(value + size, size)


def kernel(
    len_hbm, start_hbm, q_hbm, k_hbm, key_out, tok_out,
    len_ref, start_ref, qloc, kloc, qbuf, kbuf, sbuf, barred, hot, msub, lsub, lse, part, got,
    loc_sem, ready, qs, qr, ks, kr, zs, zr, ss, sr, ps, pr,
):
    x, z, y, hd = (lax.axis_index(a) for a in AXES)
    f32, bf16 = jnp.float32, jnp.bfloat16

    def share_of(ref, px, py):
        b, g = px // 2, lax.rem(px, 2)
        lanes = pl.multiple_of(g * (NY * HALF * D) + py * (HALF * D), HALF * D)
        return ref.at[b, :, pl.ds(lanes, HALF * D)]

    def keys_of(ref, px):
        b, g = px // 2, lax.rem(px, 2)
        return ref.at[b, :, pl.ds(pl.multiple_of(g * D, D), D)]

    local = [
        pltpu.make_async_copy(q_hbm, qloc, loc_sem.at[0]),
        pltpu.make_async_copy(k_hbm, kloc, loc_sem.at[1]),
        pltpu.make_async_copy(share_of(q_hbm, x, y), qbuf.at[z, x, y], loc_sem.at[2]),
        pltpu.make_async_copy(keys_of(k_hbm, x), kbuf.at[x * NY + y], loc_sem.at[3]),
        pltpu.make_async_copy(len_hbm, len_ref, loc_sem.at[4]),
        pltpu.make_async_copy(start_hbm, start_ref, loc_sem.at[5]),
    ]
    for copy in local:
        copy.start()

    barrier = pltpu.get_barrier_semaphore()
    everywhere = PLANE + ((0, 0),)
    beside = [(x, wrap(z + dz, NZ), y, hd) for dz in (1, -1)]
    heads_here = [(x, z, y, wrap(hd + dh, NH)) for dh in range(1, NH)]
    partners = beside + [(wrap(x + dx, NX), z, wrap(y + dy, NY), hd) for dx, dy in PLANE] + heads_here
    for partner in partners:
        pl.semaphore_signal(barrier, inc=1, device_id=partner, device_id_type=MESH)
    local[0].wait()
    pl.semaphore_wait(barrier, len(partners))
    for partner in beside:
        pl.semaphore_signal(ready.at[0], inc=1, device_id=partner, device_id_type=MESH)
    for partner in heads_here:
        pl.semaphore_signal(ready.at[1], inc=1, device_id=partner, device_id_type=MESH)

    def remote(src, dst, send, recv, device):
        return pltpu.make_async_remote_copy(
            src_ref=src, dst_ref=dst, send_sem=send, recv_sem=recv,
            device_id=device, device_id_type=MESH,
        )

    started = []

    def start(copy, apart=True):
        copy.start()
        if apart:
            started.append(copy)

    sends = [0]

    def q_start(dz, dx, dy):
        px, py = wrap(x + dx, NX), wrap(y + dy, NY)
        start(remote(
            share_of(qloc, px, py), qbuf.at[z, x, y], qs.at[sends[0]], qr.at[ARRIVAL[-dz], x, y],
            (px, wrap(z + dz, NZ), py, hd),
        ))
        sends[0] += 1

    def k_start(dx, dy):
        px, py = wrap(x + dx, NX), wrap(y + dy, NY)
        n = PLANE.index((dx, dy))
        start(remote(keys_of(kloc, px), kbuf.at[x * NY + y], ks.at[n], kr.at[x, y], (px, z, py, hd)))

    for dx, dy in PLANE:
        q_start(0, dx, dy)
    for dz in (1, -1):
        q_start(dz, 0, 0)
    for copy in local[1:]:
        copy.wait()
    for dx, dy in FIRST_KEYS:
        k_start(dx, dy)
    pl.semaphore_wait(ready.at[0], len(beside))
    for dx, dy in PLANE:
        for dz in (1, -1):
            q_start(dz, dx, dy)
    for dx, dy in KEY_ORDER:
        if (dx, dy) not in FIRST_KEYS:
            k_start(dx, dy)

    def q_wait(off, dx):
        for dy in (0, 1):
            if (off, dx, dy) != (0, 0, 0):
                px, py, pz = wrap(x + dx, NX), wrap(y + dy, NY), wrap(z + off, NZ)
                remote(
                    share_of(qloc, px, py), qbuf.at[pz, px, py], qs.at[0], qr.at[ARRIVAL[off], px, py],
                    (px, wrap(z + 1, NZ), py, hd),
                ).wait_recv()

    b = x // 2
    start_pos = start_ref[b]
    first_pos = len_ref[b] - QLEN
    lane = lax.broadcasted_iota(jnp.int32, (1, D), 1)
    token = lax.rem(lane, TOKENS)
    inner = NY * TOK
    lane_pos = first_pos + (token // inner) * (NZ * inner) + lax.rem(token, inner) + (lane // TOKENS) * inner

    def mask(n, carry):
        pos = (((n // NY) * NZ + z) * NY + lax.rem(n, NY)) * KEYS
        pos = pos + lax.broadcasted_iota(jnp.int32, (KEYS, D), 0)
        limit = jnp.where(pos >= start_pos, pos, jnp.int32(2**30))
        for m in range(NZ // SHARE):
            barred[m, n] = jnp.where(limit <= lane_pos + m * SHARE * inner, 0.0, FILL).astype(bf16)
        return carry

    lax.fori_loop(0, BLOCKS, mask, 0)
    row = lax.rem(lax.broadcasted_iota(jnp.int32, (ROWS, D), 0), TOKENS)
    for m in range(SHARE):
        column = lax.broadcasted_iota(jnp.int32, (ROWS, D), 1) - m * TOKENS
        hot[m] = jnp.where(row == column, 1.0, 0.0).astype(bf16)

    def z_copy(off, i, dz, n):
        slot, px = wrap(z + off, NZ), wrap(x + STRIDES[i], NX)
        there = off - dz
        j = ARRIVAL[there] if there in ARRIVAL else ARRIVAL[-there]
        return remote(
            qbuf.at[slot, px], qbuf.at[slot, px], zs.at[n], zr.at[j, i], (x, wrap(z + dz, NZ), y, hd)
        )

    def z_wait(off, i):
        slot, px = wrap(z + off, NZ), wrap(x + STRIDES[i], NX)
        remote(
            qbuf.at[slot, px], qbuf.at[slot, px], zs.at[0], zr.at[ARRIVAL[off], i],
            (x, wrap(z + 1, NZ), y, hd),
        ).wait_recv()

    sends = [0]

    def z_start(off, i, dz):
        start(z_copy(off, i, dz, sends[0]))
        sends[0] += 1

    def z_forward(i):
        for side in (1, -1):
            z_wait(side * 2, i)
            z_start(side * 2, i, -side)
        if i == NX - 1:
            for k in range(NX):
                side = 1 if k % 2 == 0 else -1
                z_start(side * 2, k, -2 * side)

    for i, dx in enumerate(STRIDES):
        for side in (1, -1):
            q_wait(side, dx)
            z_start(side, i, -side)
    for dx in STRIDES:
        q_wait(0, dx)

    def rows_of(c):
        wide = qbuf[c].astype(f32).reshape(BLOCKS * TOK, HALF * D)
        q = jnp.concatenate([wide[:, h * D:(h + 1) * D] for h in range(HALF)], axis=0).astype(bf16)
        return jnp.concatenate([q, hot[lax.rem(c, SHARE)]], axis=1)

    def score(c, q, n):
        k = jnp.concatenate([kbuf[n], barred[c // SHARE, n]], axis=1)
        s = lax.dot_general(k, q, (((1,), (1,)), ((), ())), preferred_element_type=f32)
        top = jnp.max(s, axis=0, keepdims=True)
        e = jnp.exp2((s - top) * SCALE2)
        sbuf[c, n] = e
        msub[c, pl.ds(n, 1), :] = top
        lsub[c, pl.ds(n, 1), :] = jnp.sum(e, axis=0, keepdims=True)

    def merge(c):
        tops = msub[c] * SCALE2
        top = jnp.max(tops, axis=0, keepdims=True)
        total = jnp.sum(lsub[c] * jnp.exp2(tops - top), axis=0, keepdims=True)
        lse[z, pl.ds(c, 1), :] = top + jnp.log2(total)

    near = [(wrap(z + off, NZ), rows_of(wrap(z + off, NZ))) for off in NEAR]
    for n, (dx, dy) in enumerate(((0, 0),) + KEY_ORDER):
        px, py = wrap(x + dx, NX), wrap(y + dy, NY)
        if n > 0:
            remote(
                keys_of(kloc, px), kbuf.at[px * NY + py], ks.at[0], kr.at[px, py], (px, z, py, hd)
            ).wait_recv()
        for c, q in near:
            score(c, q, px * NY + py)
        for i in range(NX):
            if n == FORWARD_AT[i]:
                z_forward(i)
    for offs in GROUPS:
        for off in offs:
            if abs(off) > 2:
                for i in range(NX):
                    z_wait(off, i)
        far = [(wrap(z + off, NZ), rows_of(wrap(z + off, NZ))) for off in offs]
        for c, q in far:
            for n in range(BLOCKS):
                score(c, q, n)
        if 2 in offs:
            for off in NEAR:
                merge(wrap(z + off, NZ))
        for off in offs:
            merge(wrap(z + off, NZ))

    for dz in (4, 3, -3, 2, -2, 1, -1):
        start(remote(lse.at[z], lse.at[z], ss.at[0], sr.at[0], (x, wrap(z + dz, NZ), y, hd)), False)
    others = lse.at[pl.ds(0, NZ - 1)]
    stats = remote(others, others, ss.at[0], sr.at[0], (x, wrap(z + 1, NZ), y, hd))
    for copy in started:
        copy.wait_send()
    started.clear()
    pl.semaphore_wait(ready.at[1], len(heads_here))
    stats.wait_recv()
    every = [lse[k] for k in range(NZ)]
    peak = functools.reduce(jnp.maximum, every)
    whole = peak + jnp.log2(sum(jnp.exp2(v - peak) for v in every))
    for c in range(NZ):
        msub[c] = jnp.exp2(msub[c] * SCALE2 - whole[c:c + 1])

    ones = jnp.ones((16, 2 * D), bf16)

    def weigh(n):
        parts = []
        for half in range(2):
            rows = pl.ds(half * D, D)
            acc = jnp.zeros((D, D), f32)
            for c in range(NZ):
                w = msub[c, pl.ds(n, 1), :]
                acc = acc + sbuf[c, n, rows, :D] * w[:, :D]
                acc = acc + sbuf[c, n, rows, D:] * w[:, D:]
            high = acc.astype(bf16)
            low = (acc - high.astype(f32)).astype(bf16)
            parts.append(jnp.concatenate([high, low], axis=1))
        return lax.dot_general(
            ones, jnp.concatenate(parts, axis=0), (((1,), (1,)), ((), ())), preferred_element_type=f32
        )[0:1]

    def send_sums(dx, dy, sums):
        px, py = wrap(x + dx, NX), wrap(y + dy, NY)
        if (dx, dy) == (0, 0):
            got[hd, x, y] = sums
        part[px * NY + py] = sums
        for dh in (3, 1, 2, 0):
            if (dx, dy, dh) != (0, 0, 0):
                start(remote(
                    part.at[px * NY + py], got.at[hd, x, y], ps.at[0], pr.at[0],
                    (px, z, py, wrap(hd + dh, NH)),
                ), False)

    held = None
    for dx, dy in everywhere:
        sums = weigh(wrap(x + dx, NX) * NY + wrap(y + dy, NY))
        if held is not None:
            send_sums(*held)
        held = (dx, dy, sums)
    send_sums(*held)
    every_sum = got.reshape(NH * BLOCKS, 1, KEYS).at[pl.ds(0, NH * BLOCKS - 1)]
    returned = remote(every_sum, every_sum, ps.at[0], pr.at[0], (x, wrap(z + 1, NZ), y, hd))
    returned.wait_recv()

    heads = KVH // NH
    for request in range(2):
        total = None
        for k in range(NH):
            for g in range(heads):
                pair = request * heads + g
                sums = got[k, pair, 0] + got[k, pair, 1]
                total = sums if total is None else total + sums
        tok_out[request:request + 1] = total
        for g in range(heads):
            pair = request * heads + g
            key_out[request, g:g + 1] = got[hd, pair, 0] + got[hd, pair, 1]

    for copy in started + [stats, returned]:
        copy.wait_send()


def body(queries, keys, lengths, starts):
    f32, bf16 = jnp.float32, jnp.bfloat16
    dma = pltpu.SemaphoreType.DMA
    vmem = pltpu.VMEM
    return pl.pallas_call(
        kernel,
        out_shape=(
            jax.ShapeDtypeStruct((2, KVH // NH, KEYS), f32),
            jax.ShapeDtypeStruct((2, KEYS), f32),
        ),
        in_specs=[pl.BlockSpec(memory_space=pltpu.HBM)] * 4,
        out_specs=(pl.BlockSpec(memory_space=vmem), pl.BlockSpec(memory_space=vmem)),
        scratch_shapes=[
            pltpu.SMEM((2,), jnp.int32),
            pltpu.SMEM((2,), jnp.int32),
            vmem(queries.shape, bf16),
            vmem(keys.shape, bf16),
            vmem((NZ, NX, NY, TOK, HALF * D), bf16),
            vmem((BLOCKS, KEYS, D), bf16),
            vmem((NZ, BLOCKS, KEYS, ROWS), f32),
            vmem((NZ // SHARE, BLOCKS, KEYS, D), bf16),
            vmem((SHARE, ROWS, D), bf16),
            vmem((NZ, BLOCKS, ROWS), f32),
            vmem((NZ, BLOCKS, ROWS), f32),
            vmem((NZ, NZ, ROWS), f32),
            vmem((BLOCKS, 1, KEYS), f32),
            vmem((NH, NX, NY, 1, KEYS), f32),
            dma((6,)),
            pltpu.SemaphoreType.REGULAR((2,)),
            dma((3 * BLOCKS - 1,)), dma((3, NX, NY)),
            dma((len(PLANE),)), dma((NX, NY)),
            dma((5 * NX,)), dma((NZ, NX)),
            dma((1,)), dma((1,)),
            dma((1,)), dma((1,)),
        ],
        compiler_params=pltpu.CompilerParams(
            collective_id=0, has_side_effects=True, vmem_limit_bytes=67043328
        ),
        name="key_scores",
    )(lengths, starts, queries, keys)


def solution(mesh):
    torus = Mesh(mesh.devices.reshape(NX, NZ, NY, NH), AXES)
    in_specs = (P(None, SEQ, "head"), P(None, SEQ, "head"), P(), P())
    out_specs = (P(None, "head", SEQ), P(None, SEQ))
    return jax.shard_map(body, mesh=torus, in_specs=in_specs, out_specs=out_specs, check_vma=False)
```

```python
import functools
import math

import jax
import jax.numpy as jnp
from jax import lax
from jax.experimental import pallas as pl
from jax.experimental.pallas import tpu as pltpu
from jax.sharding import Mesh
from jax.sharding import PartitionSpec as P

H = 64
KVH = 8
D = 128
QLEN = 512
SEQ = ("seq_0", "seq_1", "seq_2")
AXES = SEQ + ("head",)
NX, NZ, NY, NH = 4, 8, 2, 4
TOK = 8
KEYS = 256
HALF = H // KVH // NY
ROWS = NX * NY * TOK * HALF
BLOCKS = NX * NY
TOKENS = BLOCKS * TOK
SHARE = D // TOKENS
FILL = -1e30
SCALE2 = D**-0.5 * math.log2(math.e)
MESH = pl.DeviceIdType.MESH
PLANE = tuple((dx, dy) for dx in (2, 1, 3, 0) for dy in (1, 0) if (dx, dy) != (0, 0))
OFFSETS = (0, 1, -1, 2, -2, 3, -3, 4)
ARRIVAL = {off: j for j, off in enumerate(OFFSETS)}
STRIDES = (0, 1, 3, 2)
EARLY = 5
NEAR = (0, 1, -1)
GROUPS = ((2,), (-2,), (3,), (-3,), (4,))
FORWARD_AT = (4, 4, 4, 4)
KEY_ORDER = ((0, 1), (3, 0), (1, 0), (3, 1), (1, 1), (2, 0), (2, 1))
FIRST_KEYS = KEY_ORDER[:3]


def wrap(value, size):
    return lax.rem(value + size, size)


def kernel(
    len_hbm, start_hbm, q_hbm, k_hbm, key_out, tok_out,
    len_ref, start_ref, qloc, kloc, qbuf, kbuf, sbuf, barred, hot, msub, lsub, early, late, part, got,
    loc_sem, ready, qs, qr, ks, kr, zs, zr, ss, sr, ps, pr,
):
    x, z, y, hd = (lax.axis_index(a) for a in AXES)
    f32, bf16 = jnp.float32, jnp.bfloat16

    def share_of(ref, px, py):
        b, g = px // 2, lax.rem(px, 2)
        lanes = pl.multiple_of(g * (NY * HALF * D) + py * (HALF * D), HALF * D)
        return ref.at[b, :, pl.ds(lanes, HALF * D)]

    def keys_of(ref, px):
        b, g = px // 2, lax.rem(px, 2)
        return ref.at[b, :, pl.ds(pl.multiple_of(g * D, D), D)]

    local = [
        pltpu.make_async_copy(q_hbm, qloc, loc_sem.at[0]),
        pltpu.make_async_copy(k_hbm, kloc, loc_sem.at[1]),
        pltpu.make_async_copy(share_of(q_hbm, x, y), qbuf.at[z, x, y], loc_sem.at[2]),
        pltpu.make_async_copy(keys_of(k_hbm, x), kbuf.at[x * NY + y], loc_sem.at[3]),
        pltpu.make_async_copy(len_hbm, len_ref, loc_sem.at[4]),
        pltpu.make_async_copy(start_hbm, start_ref, loc_sem.at[5]),
    ]
    for copy in local:
        copy.start()

    barrier = pltpu.get_barrier_semaphore()
    everywhere = PLANE + ((0, 0),)
    beside = [(x, wrap(z + dz, NZ), y, hd) for dz in (1, -1)]
    heads_here = [(x, z, y, wrap(hd + dh, NH)) for dh in range(1, NH)]
    partners = beside + [(wrap(x + dx, NX), z, wrap(y + dy, NY), hd) for dx, dy in PLANE] + heads_here
    for partner in partners:
        pl.semaphore_signal(barrier, inc=1, device_id=partner, device_id_type=MESH)
    local[0].wait()
    pl.semaphore_wait(barrier, len(partners))
    for partner in beside:
        pl.semaphore_signal(ready.at[0], inc=1, device_id=partner, device_id_type=MESH)
    for partner in heads_here:
        pl.semaphore_signal(ready.at[1], inc=1, device_id=partner, device_id_type=MESH)

    def remote(src, dst, send, recv, device):
        return pltpu.make_async_remote_copy(
            src_ref=src, dst_ref=dst, send_sem=send, recv_sem=recv,
            device_id=device, device_id_type=MESH,
        )

    started = []

    def start(copy, apart=True):
        copy.start()
        if apart:
            started.append(copy)

    sends = [0]

    def q_start(dz, dx, dy):
        px, py = wrap(x + dx, NX), wrap(y + dy, NY)
        start(remote(
            share_of(qloc, px, py), qbuf.at[z, x, y], qs.at[sends[0]], qr.at[ARRIVAL[-dz], x, y],
            (px, wrap(z + dz, NZ), py, hd),
        ))
        sends[0] += 1

    def k_start(dx, dy):
        px, py = wrap(x + dx, NX), wrap(y + dy, NY)
        n = PLANE.index((dx, dy))
        start(remote(keys_of(kloc, px), kbuf.at[x * NY + y], ks.at[n], kr.at[x, y], (px, z, py, hd)))

    for dx, dy in PLANE:
        q_start(0, dx, dy)
    for dz in (1, -1):
        q_start(dz, 0, 0)
    for copy in local[1:]:
        copy.wait()
    for dx, dy in FIRST_KEYS:
        k_start(dx, dy)
    pl.semaphore_wait(ready.at[0], len(beside))
    for dx, dy in PLANE:
        for dz in (1, -1):
            q_start(dz, dx, dy)
    for dx, dy in KEY_ORDER:
        if (dx, dy) not in FIRST_KEYS:
            k_start(dx, dy)

    def q_wait(off, dx):
        for dy in (0, 1):
            if (off, dx, dy) != (0, 0, 0):
                px, py, pz = wrap(x + dx, NX), wrap(y + dy, NY), wrap(z + off, NZ)
                remote(
                    share_of(qloc, px, py), qbuf.at[pz, px, py], qs.at[0], qr.at[ARRIVAL[off], px, py],
                    (px, wrap(z + 1, NZ), py, hd),
                ).wait_recv()

    b = x // 2
    start_pos = start_ref[b]
    first_pos = len_ref[b] - QLEN
    lane = lax.broadcasted_iota(jnp.int32, (1, D), 1)
    token = lax.rem(lane, TOKENS)
    inner = NY * TOK
    lane_pos = first_pos + (token // inner) * (NZ * inner) + lax.rem(token, inner) + (lane // TOKENS) * inner

    def mask(n, carry):
        pos = (((n // NY) * NZ + z) * NY + lax.rem(n, NY)) * KEYS
        pos = pos + lax.broadcasted_iota(jnp.int32, (KEYS, D), 0)
        limit = jnp.where(pos >= start_pos, pos, jnp.int32(2**30))
        for m in range(NZ // SHARE):
            barred[m, n] = jnp.where(limit <= lane_pos + m * SHARE * inner, 0.0, FILL).astype(bf16)
        return carry

    lax.fori_loop(0, BLOCKS, mask, 0)
    row = lax.rem(lax.broadcasted_iota(jnp.int32, (ROWS, D), 0), TOKENS)
    for m in range(SHARE):
        column = lax.broadcasted_iota(jnp.int32, (ROWS, D), 1) - m * TOKENS
        hot[m] = jnp.where(row == column, 1.0, 0.0).astype(bf16)

    def z_copy(off, i, dz, n):
        slot, px = wrap(z + off, NZ), wrap(x + STRIDES[i], NX)
        there = off - dz
        j = ARRIVAL[there] if there in ARRIVAL else ARRIVAL[-there]
        return remote(
            qbuf.at[slot, px], qbuf.at[slot, px], zs.at[n], zr.at[j, i], (x, wrap(z + dz, NZ), y, hd)
        )

    def z_wait(off, i):
        slot, px = wrap(z + off, NZ), wrap(x + STRIDES[i], NX)
        remote(
            qbuf.at[slot, px], qbuf.at[slot, px], zs.at[0], zr.at[ARRIVAL[off], i],
            (x, wrap(z + 1, NZ), y, hd),
        ).wait_recv()

    sends = [0]

    def z_start(off, i, dz):
        start(z_copy(off, i, dz, sends[0]))
        sends[0] += 1

    def z_forward(i):
        for side in (1, -1):
            z_wait(side * 2, i)
            z_start(side * 2, i, -side)
        if i == NX - 1:
            for k in range(NX):
                side = 1 if k % 2 == 0 else -1
                z_start(side * 2, k, -2 * side)

    for i, dx in enumerate(STRIDES):
        for side in (1, -1):
            q_wait(side, dx)
            z_start(side, i, -side)
    for dx in STRIDES:
        q_wait(0, dx)

    def rows_of(c):
        wide = qbuf[c].astype(f32).reshape(BLOCKS * TOK, HALF * D)
        q = jnp.concatenate([wide[:, h * D:(h + 1) * D] for h in range(HALF)], axis=0).astype(bf16)
        return jnp.concatenate([q, hot[lax.rem(c, SHARE)]], axis=1)

    def score(c, q, n):
        k = jnp.concatenate([kbuf[n], barred[c // SHARE, n]], axis=1)
        s = lax.dot_general(k, q, (((1,), (1,)), ((), ())), preferred_element_type=f32)
        top = jnp.max(s, axis=0, keepdims=True)
        e = jnp.exp2((s - top) * SCALE2)
        sbuf[c, n] = e
        msub[c, pl.ds(n, 1), :] = top
        lsub[c, pl.ds(n, 1), :] = jnp.sum(e, axis=0, keepdims=True)

    def merge(off):
        c, j = wrap(z + off, NZ), ARRIVAL[off]
        tops = msub[c] * SCALE2
        top = jnp.max(tops, axis=0, keepdims=True)
        total = jnp.sum(lsub[c] * jnp.exp2(tops - top), axis=0, keepdims=True)
        if j < EARLY:
            early[z, j] = top + jnp.log2(total)
        else:
            late[z, j - EARLY] = top + jnp.log2(total)

    def send_stats(rows, k):
        for dz in (4, 3, -3, 2, -2, 1, -1):
            start(remote(rows.at[z], rows.at[z], ss.at[k], sr.at[k], (x, wrap(z + dz, NZ), y, hd)), False)
        others = rows.at[pl.ds(0, NZ - 1)]
        return remote(others, others, ss.at[k], sr.at[k], (x, wrap(z + 1, NZ), y, hd))

    near = [(wrap(z + off, NZ), rows_of(wrap(z + off, NZ))) for off in NEAR]
    for n, (dx, dy) in enumerate(((0, 0),) + KEY_ORDER):
        px, py = wrap(x + dx, NX), wrap(y + dy, NY)
        if n > 0:
            remote(
                keys_of(kloc, px), kbuf.at[px * NY + py], ks.at[0], kr.at[px, py], (px, z, py, hd)
            ).wait_recv()
        for c, q in near:
            score(c, q, px * NY + py)
        for i in range(NX):
            if n == FORWARD_AT[i]:
                z_forward(i)
    for offs in GROUPS:
        for off in offs:
            if abs(off) > 2:
                for i in range(NX):
                    z_wait(off, i)
            if off == 3:
                stats_early = send_stats(early, 0)
        far = [(wrap(z + off, NZ), rows_of(wrap(z + off, NZ))) for off in offs]
        for c, q in far:
            for n in range(BLOCKS):
                score(c, q, n)
        if 2 in offs:
            for off in NEAR:
                merge(off)
        for off in offs:
            merge(off)

    stats = send_stats(late, 1)
    for copy in started:
        copy.wait_send()
    started.clear()
    pl.semaphore_wait(ready.at[1], len(heads_here))
    stats_early.wait_recv()
    stats.wait_recv()
    for off in OFFSETS:
        every = []
        for dz in OFFSETS:
            j = ARRIVAL[(off - dz + NZ // 2 - 1) % NZ - NZ // 2 + 1]
            source = wrap(z + dz, NZ)
            every.append(early[source, j] if j < EARLY else late[source, j - EARLY])
        peak = functools.reduce(jnp.maximum, every)
        whole = peak + jnp.log2(sum(jnp.exp2(v - peak) for v in every))
        c = wrap(z + off, NZ)
        msub[c] = jnp.exp2(msub[c] * SCALE2 - whole)

    ones = jnp.ones((16, 2 * D), bf16)

    def weigh(n):
        parts = []
        for half in range(2):
            rows = pl.ds(half * D, D)
            acc = jnp.zeros((D, D), f32)
            for c in range(NZ):
                w = msub[c, pl.ds(n, 1), :]
                acc = acc + sbuf[c, n, rows, :D] * w[:, :D]
                acc = acc + sbuf[c, n, rows, D:] * w[:, D:]
            high = acc.astype(bf16)
            low = (acc - high.astype(f32)).astype(bf16)
            parts.append(jnp.concatenate([high, low], axis=1))
        return lax.dot_general(
            ones, jnp.concatenate(parts, axis=0), (((1,), (1,)), ((), ())), preferred_element_type=f32
        )[0:1]

    def send_sums(dx, dy, sums):
        px, py = wrap(x + dx, NX), wrap(y + dy, NY)
        if (dx, dy) == (0, 0):
            got[hd, x, y] = sums
        part[px * NY + py] = sums
        for dh in (2, 3, 1, 0):
            if (dx, dy, dh) != (0, 0, 0):
                start(remote(
                    part.at[px * NY + py], got.at[hd, x, y], ps.at[0], pr.at[0],
                    (px, z, py, wrap(hd + dh, NH)),
                ), False)

    held = None
    for dx, dy in everywhere:
        sums = weigh(wrap(x + dx, NX) * NY + wrap(y + dy, NY))
        if held is not None:
            send_sums(*held)
        held = (dx, dy, sums)
    send_sums(*held)
    every_sum = got.reshape(NH * BLOCKS, 1, KEYS).at[pl.ds(0, NH * BLOCKS - 1)]
    returned = remote(every_sum, every_sum, ps.at[0], pr.at[0], (x, wrap(z + 1, NZ), y, hd))
    returned.wait_recv()

    heads = KVH // NH
    for request in range(2):
        total = None
        for k in range(NH):
            for g in range(heads):
                pair = request * heads + g
                sums = got[k, pair, 0] + got[k, pair, 1]
                total = sums if total is None else total + sums
        tok_out[request:request + 1] = total
        for g in range(heads):
            pair = request * heads + g
            key_out[request, g:g + 1] = got[hd, pair, 0] + got[hd, pair, 1]

    for copy in started + [stats_early, stats, returned]:
        copy.wait_send()


def body(queries, keys, lengths, starts):
    f32, bf16 = jnp.float32, jnp.bfloat16
    dma = pltpu.SemaphoreType.DMA
    vmem = pltpu.VMEM
    return pl.pallas_call(
        kernel,
        out_shape=(
            jax.ShapeDtypeStruct((2, KVH // NH, KEYS), f32),
            jax.ShapeDtypeStruct((2, KEYS), f32),
        ),
        in_specs=[pl.BlockSpec(memory_space=pltpu.HBM)] * 4,
        out_specs=(pl.BlockSpec(memory_space=vmem), pl.BlockSpec(memory_space=vmem)),
        scratch_shapes=[
            pltpu.SMEM((2,), jnp.int32),
            pltpu.SMEM((2,), jnp.int32),
            vmem(queries.shape, bf16),
            vmem(keys.shape, bf16),
            vmem((NZ, NX, NY, TOK, HALF * D), bf16),
            vmem((BLOCKS, KEYS, D), bf16),
            vmem((NZ, BLOCKS, KEYS, ROWS), f32),
            vmem((NZ // SHARE, BLOCKS, KEYS, D), bf16),
            vmem((SHARE, ROWS, D), bf16),
            vmem((NZ, BLOCKS, ROWS), f32),
            vmem((NZ, BLOCKS, ROWS), f32),
            vmem((NZ, EARLY, 1, ROWS), f32),
            vmem((NZ, NZ - EARLY, 1, ROWS), f32),
            vmem((BLOCKS, 1, KEYS), f32),
            vmem((NH, NX, NY, 1, KEYS), f32),
            dma((6,)),
            pltpu.SemaphoreType.REGULAR((2,)),
            dma((3 * BLOCKS - 1,)), dma((3, NX, NY)),
            dma((len(PLANE),)), dma((NX, NY)),
            dma((5 * NX,)), dma((NZ, NX)),
            dma((2,)), dma((2,)),
            dma((1,)), dma((1,)),
        ],
        compiler_params=pltpu.CompilerParams(
            collective_id=0, has_side_effects=True, vmem_limit_bytes=67043328
        ),
        name="key_scores",
    )(lengths, starts, queries, keys)


def solution(mesh):
    torus = Mesh(mesh.devices.reshape(NX, NZ, NY, NH), AXES)
    in_specs = (P(None, SEQ, "head"), P(None, SEQ, "head"), P(), P())
    out_specs = (P(None, "head", SEQ), P(None, SEQ))
    return jax.shard_map(body, mesh=torus, in_specs=in_specs, out_specs=out_specs, check_vma=False)
```
